128 devices in a mesh: samp: 16 (over z, y_lo, core), var: 8 (over x, y_hi).
Axes of the slice: x: 4, y: 4 (y_hi: 2, y_lo: 2; y = y_hi * 2 + y_lo), z: 4, core: 2. Of those that a mesh axis runs over, the one named last changes fastest.
Arguments:
- hap_words: int32 [2, 1024, 1024], P(None, 'samp', 'var'), may hold values from 0 to 1073741823
- total_counts: int32 [30720, 8192], P('samp', 'var'), may hold values from 0 to 4999
- allele_one: int32 [30720, 8192], P('samp', 'var'), may hold values from 0 to 299
- allele_two: int32 [30720, 8192], P('samp', 'var'), may hold values from 0 to 299
Outputs:
- z_total: float32 [1024, 8192], P('samp', 'var')
- z_allelic: float32 [1024, 8192], P('samp', 'var')
The draws below stay inside these ranges and needn't reach their ends.
Inputs may be any that keep to these rules, and one draw needn't show every extreme that they name: Bit k, for k below 30, of hap_words[c, j, v] is haplotype c of sample 30 * j + k at variant v; higher bits are zero.
All inputs are finite; a program needn't handle non-finite values.
Results may differ from the reference program's by a relative error of at most 0.0003.
The reference program's roundings to bfloat16 on the way count: a program that leaves them out, or rounds other values in their place, can miss the bound.
Values sent between devices are 32-bit elements; how exact they have to be, the bound alone decides.
A program may use at most 192 MiB of HBM per device.

```python
import jax
import jax.numpy as jnp
from jax import lax

BITS = 30
GENES = 8192
SWORDS = 1024
SAMPLES = 30720
VARIANTS = 1024


def with_ends(array, own_key, low, high):
    longest = array.shape.index(max(array.shape))
    spots = []
    for shift in (0, 1):
        where = [jax.random.randint(jax.random.fold_in(own_key, axis), (), 0, length) for axis, length in enumerate(array.shape)]
        where[longest] = (where[longest] + shift) % array.shape[longest]
        spots.append(tuple(where))
    return array.at[spots[0]].set(low).at[spots[1]].set(high)


def setup_inputs(seed: int = 0) -> dict:
    seeds = jax.random.split(jax.random.key(seed), 5)
    hap_words = with_ends(jax.random.randint(seeds[0], (2, SWORDS, VARIANTS), 0, 2 ** BITS), jax.random.fold_in(seeds[0], 1), 0, (2 ** BITS) - 1).astype(jnp.int32)
    total_counts = with_ends(jax.random.randint(seeds[1], (SAMPLES, GENES), 0, 5000), jax.random.fold_in(seeds[1], 1), 0, 4999).astype(jnp.int32)
    allele_one = with_ends(jax.random.randint(seeds[2], (SAMPLES, GENES), 0, 300), jax.random.fold_in(seeds[2], 1), 0, 299).astype(jnp.int32)
    allele_two = with_ends(jax.random.randint(seeds[3], (SAMPLES, GENES), 0, 300), jax.random.fold_in(seeds[3], 1), 0, 299).astype(jnp.int32)
    return dict(hap_words=hap_words, total_counts=total_counts, allele_one=allele_one, allele_two=allele_two)


def unpack(packed):
    shifts = jnp.arange(BITS, dtype=jnp.int32)
    bit_table = jnp.bitwise_and(jnp.right_shift(packed[:, :, None, :], shifts[None, None, :, None]), 1)
    return bit_table.reshape(2, packed.shape[1] * BITS, packed.shape[2])

def features(total_part, one_part, two_part):
    log_total = jnp.log1p(total_part.astype(jnp.float32))
    one_plus = one_part.astype(jnp.float32) + 1.0
    two_plus = two_part.astype(jnp.float32) + 1.0
    log_ratio = jnp.log(one_plus / two_plus)
    weight = 1.0 / (1.0 / one_plus + 1.0 / two_plus)
    return (log_total, (weight * log_ratio).astype(jnp.bfloat16), weight.astype(jnp.bfloat16))

def finish(cross_total, cross_allelic, het_weight, dos_sum, dos_sq, gene_sum, gene_sq, sample_count):
    dosage_var = dos_sq - dos_sum * dos_sum / sample_count
    gene_var = gene_sq - gene_sum * gene_sum / sample_count
    covariance = cross_total - dos_sum[:, None] * gene_sum[None, :] / sample_count
    z_total = jnp.sqrt(sample_count) * covariance / jnp.sqrt((dosage_var[:, None] + 1.0) * (gene_var[None, :] + 1.0))
    z_allelic = cross_allelic / jnp.sqrt(het_weight + 1.0)
    return (z_total, z_allelic)

def reference(hap_words, total_counts, allele_one, allele_two):
    bit_table = unpack(hap_words)
    dosage = bit_table[0] + bit_table[1] - 1
    phase_diff = bit_table[0] - bit_table[1]
    dosage_f = dosage.astype(jnp.float32)
    dos_sum = lax.optimization_barrier(jnp.sum(dosage_f, axis=0))
    dos_sq = lax.optimization_barrier(jnp.sum(dosage_f * dosage_f, axis=0))
    dosage_b = dosage.astype(jnp.bfloat16)
    phase_b = phase_diff.astype(jnp.bfloat16)
    phase_sq_b = (phase_diff * phase_diff).astype(jnp.bfloat16)
    sample_count = jnp.float32(hap_words.shape[1] * BITS)
    block_width = GENES // 8

    def one_block(block_index):
        first_col = (block_index * block_width).astype(jnp.int32)
        total_part = lax.dynamic_slice_in_dim(total_counts, first_col, block_width, 1)
        one_part = lax.dynamic_slice_in_dim(allele_one, first_col, block_width, 1)
        two_part = lax.dynamic_slice_in_dim(allele_two, first_col, block_width, 1)
        log_total, weighted_b, weight_b = features(total_part, one_part, two_part)
        cross_total = jnp.dot(dosage_b.T, log_total.astype(jnp.bfloat16), preferred_element_type=jnp.float32)
        cross_allelic = jnp.dot(phase_b.T, weighted_b, preferred_element_type=jnp.float32)
        het_weight = jnp.dot(phase_sq_b.T, weight_b, preferred_element_type=jnp.float32)
        gene_sum = lax.optimization_barrier(jnp.sum(log_total, axis=0))
        gene_sq = lax.optimization_barrier(jnp.sum(log_total * log_total, axis=0))
        return finish(cross_total, cross_allelic, het_weight, dos_sum, dos_sq, gene_sum, gene_sq, sample_count)
    total_blocks, allelic_blocks = lax.map(one_block, jnp.arange(8, dtype=jnp.int32))
    variants = hap_words.shape[2]
    z_total = jnp.moveaxis(total_blocks, 0, 1).reshape(variants, GENES)
    z_allelic = jnp.moveaxis(allelic_blocks, 0, 1).reshape(variants, GENES)
    return (z_total, z_allelic)
```

```python
import functools

import jax
import jax.numpy as jnp
from jax import lax
from jax.experimental import pallas as pl
from jax.experimental.pallas import tpu as pltpu
from jax.sharding import PartitionSpec as P

BITS = 30
ROWS_IN = 128
SLOTS = 4
LANES = 256
MESH = pl.DeviceIdType.MESH
BF16 = jnp.bfloat16
F32 = jnp.float32


def kernel(
    n_var,
    sample_count,
    hap_ref,
    total_ref,
    one_ref,
    two_ref,
    zt_ref,
    za_ref,
    hall,
    feats,
    counts,
    gacc,
    tbuf,
    lhs,
    acc,
    r0,
    r1,
    r2,
    r3,
    marg,
    mrecv,
    in_sem,
    hap_own,
    hap_send,
    hap_recv,
    s0s,
    s0r,
    s1s,
    s1r,
    s2s,
    s2r,
    s3s,
    s3r,
    ms,
    mr,
):
    samples, genes = total_ref.shape
    words = hap_ref.shape[1]
    rows = acc.shape[4]
    s = lax.axis_index("samp")
    v = lax.axis_index("var")
    c = s % 2
    y = (s // 2) % 2
    z = s // 4
    za = z + 1 - 2 * (z % 2)
    zb = 3 - z
    zc = (z + 2) % 4
    core_dev = (s + 1 - 2 * c, v)
    y_dev = (s + 2 - 4 * y, v)
    a_dev = (za * 4 + y * 2 + c, v)
    b_dev = (zb * 4 + y * 2 + c, v)
    cube = (core_dev, y_dev, a_dev, b_dev)
    oc = 1 - c
    oy = 1 - y

    n_chunks = samples // ROWS_IN

    def fetch(k, slot, which, ref):
        return pltpu.make_async_copy(
            ref.at[pl.ds(pl.multiple_of(k * ROWS_IN, ROWS_IN), ROWS_IN), :],
            counts.at[slot, which],
            in_sem.at[slot, which],
        )

    sources = (total_ref, one_ref, two_ref)
    for k in range(SLOTS - 1):
        for which, ref in enumerate(sources):
            fetch(k, k, which, ref).start()

    barrier = pltpu.get_barrier_semaphore()
    for dev in cube:
        pl.semaphore_signal(barrier, inc=1, device_id=dev, device_id_type=MESH)
    for k in range(1, n_var):
        pl.semaphore_signal(
            barrier, inc=1, device_id=(s, (v + k) % n_var), device_id_type=MESH
        )
    pl.semaphore_wait(barrier, 4 + n_var - 1)

    own = pltpu.make_async_copy(hap_ref, hall.at[v], hap_own)
    own.start()

    def hap_copy(k):
        return pltpu.make_async_remote_copy(
            src_ref=hap_ref,
            dst_ref=hall.at[v],
            send_sem=hap_send.at[k],
            recv_sem=hap_recv.at[k],
            device_id=(s, (v + k) % n_var),
            device_id_type=MESH,
        )

    def hap_arrival(k):
        return pltpu.make_async_remote_copy(
            src_ref=hap_ref,
            dst_ref=hall.at[(v + n_var - k) % n_var],
            send_sem=hap_send.at[k],
            recv_sem=hap_recv.at[k],
            device_id=(s, (v + k) % n_var),
            device_id_type=MESH,
        )

    for k in range(1, n_var):
        hap_copy(k).start()

    gacc[...] = jnp.zeros_like(gacc)

    def chunk_step(k, carry):
        slot = k % SLOTS

        @pl.when(k + SLOTS - 1 < n_chunks)
        def _():
            for which, ref in enumerate(sources):
                fetch(k + SLOTS - 1, (k + SLOTS - 1) % SLOTS, which, ref).start()

        for which, ref in enumerate(sources):
            fetch(k, slot, which, ref).wait()

        def row_step(r, carry):
            at = pl.ds(pl.multiple_of(r * 16, 16), 16)
            out = pl.ds(pl.multiple_of(k * ROWS_IN + r * 16, 16), 16)
            for lane in range(0, genes, LANES):
                cols = pl.ds(lane, LANES)
                log_total = jnp.log((counts[slot, 0, at, cols] + 1).astype(F32))
                one = (counts[slot, 1, at, cols] + 1).astype(F32)
                two = (counts[slot, 2, at, cols] + 1).astype(F32)
                weight = (one * two) / (one + two)
                weighted = weight * (jnp.log(one) - jnp.log(two))
                feats[0, out, cols] = log_total.astype(BF16)
                feats[1, out, cols] = weighted.astype(BF16)
                feats[2, out, cols] = weight.astype(BF16)
                square = log_total * log_total
                gacc[0, :, cols] += log_total[:8] + log_total[8:]
                gacc[1, :, cols] += square[:8] + square[8:]
            return carry

        lax.fori_loop(0, ROWS_IN // 16, row_step, 0)
        return carry

    lax.fori_loop(0, n_chunks, chunk_step, 0)

    own.wait()
    for k in range(1, n_var):
        hap_arrival(k).wait_recv()

    marg[0] = jnp.zeros_like(marg[0])
    marg[0, 0:1, :] = jnp.sum(gacc[0], axis=0, keepdims=True)
    marg[0, 1:2, :] = jnp.sum(gacc[1], axis=0, keepdims=True)
    for b in range(n_var):
        w0, w1 = hall[b, 0], hall[b, 1]
        bits = lax.population_count(w0) + lax.population_count(w1)
        het = lax.population_count(jnp.bitwise_xor(w0, w1))
        cols = pl.ds(b * 128, 128)
        bit_sum = jnp.sum(bits.astype(F32), axis=0, keepdims=True)
        het_sum = jnp.sum(het.astype(F32), axis=0, keepdims=True)
        marg[0, 2:3, cols] = bit_sum - float(samples)
        marg[0, 3:4, cols] = float(samples) - het_sum

    def marg_copy(k):
        return pltpu.make_async_remote_copy(
            src_ref=marg.at[k],
            dst_ref=mrecv.at[k],
            send_sem=ms.at[k],
            recv_sem=mr.at[k],
            device_id=cube[k],
            device_id_type=MESH,
        )

    def marg_finish(k):
        marg_copy(k).wait_recv()
        marg[k + 1] = marg[k] + mrecv[k]

    marg_copy(0).start()

    def send(src, dst, ss, rs, dev):
        return pltpu.make_async_remote_copy(
            src_ref=src,
            dst_ref=dst,
            send_sem=ss,
            recv_sem=rs,
            device_id=dev,
            device_id_type=MESH,
        )

    def s0(p, i, t):
        return send(acc.at[p, i, t, oc], r0.at[p, i, t], s0s.at[p, i, t], s0r.at[p, i, t], core_dev)

    def s0_finish(p, i):
        for t in range(2):
            s0(p, i, t).wait_recv()
            acc[p, i, t, c] = acc[p, i, t, c] + r0[p, i, t]

    def s1_total(i):
        return send(acc.at[0, i, oy, c], r1.at[0, i], s1s.at[0, i], s1r.at[0, i], y_dev)

    def s1_allelic(i, t):
        at = 2 * i + t
        return send(acc.at[1, i, t, c], r1.at[1, at], s1s.at[1, at], s1r.at[1, at], a_dev)

    def s1_het(i, t):
        return send(acc.at[2, i, t, c], r1.at[2, i + t], s1s.at[2, i + t], s1r.at[2, i + t], b_dev)

    def s0_then_s1(p, i):
        s0_finish(p, i)
        if p == 0:
            s1_total(i).start()
        elif p == 1:

            @pl.when(i < 2)
            def _():
                for t in range(2):
                    s1_allelic(i, t).start()
        else:

            @pl.when(i % 2 == 0)
            def _():
                for t in range(2):
                    s1_het(i, t).start()

    iota = lax.broadcasted_iota(jnp.int32, (8, 128), 0)

    def unpack(i):
        zt = jnp.where(i == 0, zc, jnp.where(i == 1, za, jnp.where(i == 2, zb, z)))
        for b in range(2):
            block = 2 * zt + b

            def word_step(g, carry):
                at = pl.ds(pl.multiple_of(g * 8, 8), 8)
                w0 = hall[block, 0, at, :]
                w1 = hall[block, 1, at, :] << 1
                parts = []
                for t in range(BITS):
                    first = 8 * t // BITS
                    last = (8 * t + 7) // BITS
                    shift = iota + (8 * t - BITS * first)
                    u0 = jnp.broadcast_to(w0[first : first + 1], (8, 128))
                    u1 = jnp.broadcast_to(w1[first : first + 1], (8, 128))
                    if last != first:
                        early = iota < BITS * last - 8 * t
                        shift = jnp.where(early, shift, shift - BITS)
                        u0 = jnp.where(early, u0, jnp.broadcast_to(w0[last : last + 1], (8, 128)))
                        u1 = jnp.where(early, u1, jnp.broadcast_to(w1[last : last + 1], (8, 128)))
                    code = ((u0 >> shift) & 1) | ((u1 >> shift) & 2)
                    parts.append(code.astype(F32))
                out = pl.ds(pl.multiple_of(g * 8 * BITS, 16), 8 * BITS)
                tbuf[out, :] = jnp.concatenate(parts, axis=0).astype(BF16)
                return carry

            lax.fori_loop(0, words // 8, word_step, 0)

            def turn_step(k, carry):
                at = pl.ds(pl.multiple_of(k * 128, 128), 128)
                centred = tbuf[at, :].T - 1.5
                het = jnp.abs(centred) < 1.0
                zero = jnp.zeros_like(centred)
                out = pl.ds(b * 128, 128)
                lhs[0, out, at] = jnp.clip(jnp.where(het, zero, centred), -1.0, 1.0)
                lhs[1, out, at] = jnp.where(het, centred * -2.0, zero)
                lhs[2, out, at] = jnp.where(het, jnp.ones_like(centred), zero)
                return carry

            lax.fori_loop(0, samples // 128, turn_step, 0)

    def matmul(p, i):
        def col_step(n, carry):
            cols = pl.ds(pl.multiple_of(n * LANES, LANES), LANES)
            res = jnp.dot(lhs[p], feats[p, :, cols], preferred_element_type=F32)
            acc[p, i, :, :, :, cols] = res.reshape(2, 2, rows, LANES)
            return carry

        lax.fori_loop(0, genes // LANES, col_step, 0)
        for t in range(2):
            s0(p, i, t).start()

    def tile_step(i, carry):
        unpack(i)

        @pl.when(i > 0)
        def _():
            s0_then_s1(0, i - 1)

        matmul(1, i)

        @pl.when(i == 0)
        def _():
            marg_finish(0)
            marg_copy(1).start()

        matmul(2, i)
        s0_then_s1(1, i)
        matmul(0, i)
        s0_then_s1(2, i)
        return carry

    lax.fori_loop(0, 4, tile_step, 0)
    s0_then_s1(0, 3)
    marg_finish(1)
    marg_copy(2).start()

    def s2_total(k):
        return send(acc.at[0, k, y, c], r2.at[0, k], s2s.at[0, k], s2r.at[0, k], a_dev)

    def s2_allelic(k):
        t = oy if k == 0 else y
        return send(acc.at[1, 2, t, c], r2.at[1, k], s2s.at[1, k], s2r.at[1, k], b_dev)

    def s2_het(k):
        return send(acc.at[2, 1 + 2 * k, oy, c], r2.at[2, k], s2s.at[2, k], s2r.at[2, k], y_dev)

    def s3_total():
        return send(acc.at[0, 2, y, c], r3.at[0], s3s.at[0], s3r.at[0], b_dev)

    def s3_allelic():
        return send(acc.at[1, 3, oy, c], r3.at[1], s3s.at[1], s3r.at[1], y_dev)

    def s3_het():
        return send(acc.at[2, 1, y, c], r3.at[2], s3s.at[2], s3r.at[2], a_dev)

    for t in range(2):
        s1_allelic(0, t).wait_recv()
        acc[1, 2, t, c] = acc[1, 2, t, c] + r1[1, t]
    s2_allelic(0).start()
    s2_allelic(1).start()
    for t in range(2):
        s1_het(0, t).wait_recv()
        acc[2, 1, t, c] = acc[2, 1, t, c] + r1[2, t]
    s2_het(0).start()
    for k in range(2):
        s1_total(k).wait_recv()
        acc[0, k, y, c] = acc[0, k, y, c] + r1[0, k]
        s2_total(k).start()
    for k in range(2, 4):
        s1_total(k).wait_recv()
        acc[0, k, y, c] = acc[0, k, y, c] + r1[0, k]
    for t in range(2):
        s1_het(2, t).wait_recv()
        acc[2, 3, t, c] = acc[2, 3, t, c] + r1[2, 2 + t]
    s2_het(1).start()
    for t in range(2):
        s1_allelic(1, t).wait_recv()
        acc[1, 3, t, c] = acc[1, 3, t, c] + r1[1, 2 + t]

    marg_finish(2)
    marg_copy(3).start()

    s2_allelic(0).wait_recv()
    acc[1, 3, oy, c] = acc[1, 3, oy, c] + r2[1, 0]
    s3_allelic().start()
    s2_het(0).wait_recv()
    acc[2, 1, y, c] = acc[2, 1, y, c] + r2[2, 0]
    s3_het().start()
    s2_total(0).wait_recv()
    acc[0, 2, y, c] = acc[0, 2, y, c] + r2[0, 0]
    s3_total().start()

    marg_finish(3)
    gene_sum = marg[4, 0:1, :]
    gene_sq = marg[4, 1:2, :]
    lane = lax.broadcasted_iota(jnp.int32, (rows, marg.shape[2]), 1)
    row = lax.broadcasted_iota(jnp.int32, (rows, marg.shape[2]), 0)
    mine = lane == row + rows * s
    dos_sum = jnp.sum(jnp.where(mine, marg[4, 2:3, :], 0.0), axis=1, keepdims=True)
    dos_sq = jnp.sum(jnp.where(mine, marg[4, 3:4, :], 0.0), axis=1, keepdims=True)
    n = sample_count
    dosage_var = dos_sq - dos_sum * dos_sum / n
    gene_var = gene_sq - gene_sum * gene_sum / n

    s2_allelic(1).wait_recv()
    s2_het(1).wait_recv()
    s2_total(1).wait_recv()
    s3_allelic().wait_recv()
    s3_het().wait_recv()
    allelic = acc[1, 3, y, c] + r2[1, 1] + r3[1]
    het_weight = acc[2, 3, y, c] + r2[2, 1] + r3[2]
    za_ref[...] = allelic / jnp.sqrt(het_weight + 1.0)
    s3_total().wait_recv()
    total = acc[0, 3, y, c] + r2[0, 1] + r3[0]
    covariance = total - dos_sum * (gene_sum / n)
    scale = jnp.sqrt((dosage_var + 1.0) * (gene_var + 1.0))
    zt_ref[...] = (n**0.5) * covariance / scale

    for k in range(1, n_var):
        hap_copy(k).wait_send()
    for k in range(4):
        marg_copy(k).wait_send()

    def drain(i, carry):
        for p in range(3):
            for t in range(2):
                s0(p, i, t).wait_send()
        s1_total(i).wait_send()
        return carry

    lax.fori_loop(0, 4, drain, 0)
    for i in range(2):
        for t in range(2):
            s1_allelic(i, t).wait_send()
            s1_het(2 * i, t).wait_send()
        s2_total(i).wait_send()
        s2_allelic(i).wait_send()
        s2_het(i).wait_send()
    s3_total().wait_send()
    s3_allelic().wait_send()
    s3_het().wait_send()


def per_device(sample_count, hap_words, total_counts, allele_one, allele_two):
    n_var = lax.axis_size("var")
    words, block = hap_words.shape[1:]
    samples, genes = total_counts.shape
    variants = block * n_var
    rows = variants // 16
    tile = variants // 4
    dma = pltpu.SemaphoreType.DMA
    out = jax.ShapeDtypeStruct((rows, genes), F32)
    return pl.pallas_call(
        functools.partial(kernel, n_var, float(sample_count)),
        out_shape=(out, out),
        in_specs=[pl.BlockSpec(memory_space=pl.ANY)] * 4,
        out_specs=(pl.BlockSpec(memory_space=pltpu.VMEM),) * 2,
        scratch_shapes=[
            pltpu.VMEM((n_var, 2, words, block), jnp.int32),
            pltpu.VMEM((3, samples, genes), BF16),
            pltpu.VMEM((SLOTS, 3, ROWS_IN, genes), jnp.int32),
            pltpu.VMEM((2, 8, genes), F32),
            pltpu.VMEM((samples, 128), BF16),
            pltpu.VMEM((3, tile, samples), BF16),
            pltpu.VMEM((3, 4, 2, 2, rows, genes), F32),
            pltpu.VMEM((3, 4, 2, rows, genes), F32),
            pltpu.VMEM((3, 4, rows, genes), F32),
            pltpu.VMEM((3, 2, rows, genes), F32),
            pltpu.VMEM((3, rows, genes), F32),
            pltpu.VMEM((5, 8, variants), F32),
            pltpu.VMEM((4, 8, variants), F32),
            dma((SLOTS, 3)),
            dma,
            dma((n_var,)),
            dma((n_var,)),
            dma((3, 4, 2)),
            dma((3, 4, 2)),
            dma((3, 4)),
            dma((3, 4)),
            dma((3, 2)),
            dma((3, 2)),
            dma((3,)),
            dma((3,)),
            dma((4,)),
            dma((4,)),
        ],
        compiler_params=pltpu.CompilerParams(
            collective_id=0,
            has_side_effects=True,
            vmem_limit_bytes=64_000_000,
        ),
    )(hap_words, total_counts, allele_one, allele_two)


def solution(mesh):
    in_specs = (P(None, "samp", "var"), P("samp", "var"), P("samp", "var"), P("samp", "var"))
    out_specs = (P("samp", "var"), P("samp", "var"))

    def whole(hap_words, total_counts, allele_one, allele_two):
        body = functools.partial(per_device, total_counts.shape[0])
        return jax.shard_map(
            body, mesh=mesh, in_specs=in_specs, out_specs=out_specs, check_vma=False
        )(hap_words, total_counts, allele_one, allele_two)

    return whole
```

```python
import functools

import jax
import jax.numpy as jnp
from jax import lax
from jax.experimental import pallas as pl
from jax.experimental.pallas import tpu as pltpu
from jax.sharding import PartitionSpec as P

BITS = 30
ROWS_IN = 128
SLOTS = 3
TURN = 5
EARLY = 3
LANES = 256
MESH = pl.DeviceIdType.MESH
BF16 = jnp.bfloat16
F32 = jnp.float32


def kernel(
    n_var,
    sample_count,
    hap_ref,
    total_ref,
    one_ref,
    two_ref,
    zt_ref,
    za_ref,
    hall,
    feats,
    counts,
    gacc,
    tbuf,
    lhs,
    acc,
    r0,
    r1,
    r2,
    r3,
    marg,
    mrecv,
    in_sem,
    hap_own,
    hap_send,
    hap_recv,
    s0s,
    s0r,
    s1s,
    s1r,
    s2s,
    s2r,
    s3s,
    s3r,
    ms,
    mr,
):
    samples, genes = total_ref.shape
    words = hap_ref.shape[1]
    rows = acc.shape[4]
    s = lax.axis_index("samp")
    v = lax.axis_index("var")
    c = s % 2
    y = (s // 2) % 2
    z = s // 4
    za = z + 1 - 2 * (z % 2)
    zb = 3 - z
    zc = (z + 2) % 4
    core_dev = (s + 1 - 2 * c, v)
    y_dev = (s + 2 - 4 * y, v)
    a_dev = (za * 4 + y * 2 + c, v)
    b_dev = (zb * 4 + y * 2 + c, v)
    cube = (core_dev, y_dev, a_dev, b_dev)
    oc = 1 - c
    oy = 1 - y

    n_chunks = samples // ROWS_IN

    def fetch(k, slot, which, ref):
        return pltpu.make_async_copy(
            ref.at[pl.ds(pl.multiple_of(k * ROWS_IN, ROWS_IN), ROWS_IN), :],
            counts.at[slot, which],
            in_sem.at[slot, which],
        )

    sources = (total_ref, one_ref, two_ref)
    for k in range(SLOTS - 1):
        for which, ref in enumerate(sources):
            fetch(k, k, which, ref).start()

    barrier = pltpu.get_barrier_semaphore()
    for dev in cube:
        pl.semaphore_signal(barrier, inc=1, device_id=dev, device_id_type=MESH)
    for k in range(1, n_var):
        pl.semaphore_signal(
            barrier, inc=1, device_id=(s, (v + k) % n_var), device_id_type=MESH
        )
    own = pltpu.make_async_copy(hap_ref, hall.at[v], hap_own)
    own.start()

    def hap_copy(k):
        return pltpu.make_async_remote_copy(
            src_ref=hap_ref,
            dst_ref=hall.at[v],
            send_sem=hap_send.at[k],
            recv_sem=hap_recv.at[k],
            device_id=(s, (v + k) % n_var),
            device_id_type=MESH,
        )

    def hap_arrival(k):
        return pltpu.make_async_remote_copy(
            src_ref=hap_ref,
            dst_ref=hall.at[(v + n_var - k) % n_var],
            send_sem=hap_send.at[k],
            recv_sem=hap_recv.at[k],
            device_id=(s, (v + k) % n_var),
            device_id_type=MESH,
        )

    gacc[...] = jnp.zeros_like(gacc)

    def chunk_step(k, carry):
        slot = k % SLOTS

        @pl.when(k + SLOTS - 1 < n_chunks)
        def _():
            for which, ref in enumerate(sources):
                fetch(k + SLOTS - 1, (k + SLOTS - 1) % SLOTS, which, ref).start()

        for which, ref in enumerate(sources):
            fetch(k, slot, which, ref).wait()

        def row_step(r, carry):
            at = pl.ds(pl.multiple_of(r * 16, 16), 16)
            out = pl.ds(pl.multiple_of(k * ROWS_IN + r * 16, 16), 16)
            for lane in range(0, genes, LANES):
                cols = pl.ds(lane, LANES)
                log_total = jnp.log((counts[slot, 0, at, cols] + 1).astype(F32))
                one = (counts[slot, 1, at, cols] + 1).astype(F32)
                two = (counts[slot, 2, at, cols] + 1).astype(F32)
                weight = (one * two) / (one + two)
                weighted = weight * (jnp.log(one) - jnp.log(two))
                feats[0, out, cols] = log_total.astype(BF16)
                feats[1, out, cols] = weighted.astype(BF16)
                feats[2, out, cols] = weight.astype(BF16)
                square = log_total * log_total
                gacc[0, :, cols] += log_total[:8] + log_total[8:]
                gacc[1, :, cols] += square[:8] + square[8:]
            return carry

        lax.fori_loop(0, ROWS_IN // 16, row_step, 0)
        return carry

    with jax.named_scope("features_a"):
        lax.fori_loop(0, EARLY, chunk_step, 0)
    with jax.named_scope("barrier"):
        pl.semaphore_wait(barrier, 4 + n_var - 1)
    for k in range(1, n_var):
        hap_copy(k).start()
    with jax.named_scope("features_b"):
        lax.fori_loop(EARLY, n_chunks, chunk_step, 0)

    with jax.named_scope("hap_wait"):
        own.wait()
        for k in range(1, n_var):
            hap_arrival(k).wait_recv()

    marg[0] = jnp.zeros_like(marg[0])
    marg[0, 0:1, :] = jnp.sum(gacc[0], axis=0, keepdims=True)
    marg[0, 1:2, :] = jnp.sum(gacc[1], axis=0, keepdims=True)
    for b in range(n_var):
        w0, w1 = hall[b, 0], hall[b, 1]
        bits = lax.population_count(w0) + lax.population_count(w1)
        het = lax.population_count(jnp.bitwise_xor(w0, w1))
        cols = pl.ds(b * 128, 128)
        bit_sum = jnp.sum(bits.astype(F32), axis=0, keepdims=True)
        het_sum = jnp.sum(het.astype(F32), axis=0, keepdims=True)
        marg[0, 2:3, cols] = bit_sum - float(samples)
        marg[0, 3:4, cols] = float(samples) - het_sum

    def marg_copy(k):
        return pltpu.make_async_remote_copy(
            src_ref=marg.at[k],
            dst_ref=mrecv.at[k],
            send_sem=ms.at[k],
            recv_sem=mr.at[k],
            device_id=cube[k],
            device_id_type=MESH,
        )

    def marg_finish(k):
        with jax.named_scope("marg_wait"):
            marg_copy(k).wait_recv()
        marg[k + 1] = marg[k] + mrecv[k]

    marg_copy(0).start()

    def send(src, dst, ss, rs, dev):
        return pltpu.make_async_remote_copy(
            src_ref=src,
            dst_ref=dst,
            send_sem=ss,
            recv_sem=rs,
            device_id=dev,
            device_id_type=MESH,
        )

    half = genes // 2
    halves = (pl.ds(0, half), pl.ds(half, half))
    whole = (pl.ds(0, genes),)

    def parts(i):
        return halves if i == 0 else whole

    def s0(p, i, t, h):
        cols = parts(i)[h]
        return send(
            acc.at[p, i, t, oc, :, cols],
            r0.at[p, i, t, :, cols],
            s0s.at[p, i, t, h],
            s0r.at[p, i, t, h],
            core_dev,
        )

    def s1(p, i, t, h):
        cols = parts(i)[h]
        if p == 0:
            src, slot, dev = (i, oy), i, y_dev
        elif p == 1:
            src, slot, dev = (i, t), 2 * i + t, a_dev
        else:
            src, slot, dev = (i, t), i + t, b_dev
        return send(
            acc.at[p, src[0], src[1], c, :, cols],
            r1.at[p, slot, :, cols],
            s1s.at[p, slot, h],
            s1r.at[p, slot, h],
            dev,
        )

    def s1_pieces(p, i):
        if p == 0:
            return (0,)
        if p == 1:
            return (0, 1) if i < 2 else ()
        return (0, 1) if i % 2 == 0 else ()

    def s0_finish(p, i, h=0):
        cols = parts(i)[h]
        for t in range(2):
            with jax.named_scope("s0_wait"):
                s0(p, i, t, h).wait_recv()
            acc[p, i, t, c, :, cols] += r0[p, i, t, :, cols]
        for t in s1_pieces(p, i):
            s1(p, i, t, h).start()

    iota = lax.broadcasted_iota(jnp.int32, (8, 128), 0)

    def unpack_words(i):
        zt = (zc, za, zb, z)[i]
        for b in range(2):
            block = 2 * zt + b

            def word_step(g, carry):
                at = pl.ds(pl.multiple_of(g * 8, 8), 8)
                w0 = hall[block, 0, at, :]
                w1 = hall[block, 1, at, :] << 1
                parts = []
                for t in range(BITS):
                    first = 8 * t // BITS
                    last = (8 * t + 7) // BITS
                    shift = iota + (8 * t - BITS * first)
                    u0 = jnp.broadcast_to(w0[first : first + 1], (8, 128))
                    u1 = jnp.broadcast_to(w1[first : first + 1], (8, 128))
                    if last != first:
                        early = iota < BITS * last - 8 * t
                        shift = jnp.where(early, shift, shift - BITS)
                        u0 = jnp.where(early, u0, jnp.broadcast_to(w0[last : last + 1], (8, 128)))
                        u1 = jnp.where(early, u1, jnp.broadcast_to(w1[last : last + 1], (8, 128)))
                    code = ((u0 >> shift) & 1) | ((u1 >> shift) & 2)
                    parts.append(code.astype(F32))
                out = pl.ds(pl.multiple_of(g * 8 * BITS, 16), 8 * BITS)
                tbuf[b, out, :] = jnp.concatenate(parts, axis=0).astype(BF16)
                return carry

            lax.fori_loop(0, words // 8, word_step, 0)

    def turn(i):
        def turn_step(k, carry):
            for b in range(2):
                for j in range(TURN):
                    at = pl.ds(pl.multiple_of(k * (TURN * 128) + j * 128, 128), 128)
                    centred = tbuf[b, at, :].T - 1.5
                    het = jnp.abs(centred) < 1.0
                    zero = jnp.zeros_like(centred)
                    out = pl.ds(b * 128, 128)
                    lhs[i, 0, out, at] = jnp.clip(jnp.where(het, zero, centred), -1.0, 1.0)
                    lhs[i, 1, out, at] = jnp.where(het, centred * -2.0, zero)
                    lhs[i, 2, out, at] = jnp.where(het, jnp.ones_like(centred), zero)
            return carry

        lax.fori_loop(0, samples // (TURN * 128), turn_step, 0)

    def matmul(p, i, h=0):
        cols = parts(i)[h]
        with jax.named_scope("matmul"):
            res = jnp.dot(lhs[i, p], feats[p, :, cols], preferred_element_type=F32)
            acc[p, i, :, :, :, cols] = res.reshape(2, 2, rows, res.shape[1])
        for t in range(2):
            s0(p, i, t, h).start()

    def s2_total(k):
        return send(acc.at[0, k, y, c], r2.at[0, k], s2s.at[0, k], s2r.at[0, k], a_dev)

    def s2_allelic(k):
        t = oy if k == 0 else y
        return send(acc.at[1, 2, t, c], r2.at[1, k], s2s.at[1, k], s2r.at[1, k], b_dev)

    def s2_het(k):
        return send(acc.at[2, 1 + 2 * k, oy, c], r2.at[2, k], s2s.at[2, k], s2r.at[2, k], y_dev)

    def s3_total():
        return send(acc.at[0, 2, y, c], r3.at[0], s3s.at[0], s3r.at[0], b_dev)

    def s3_allelic():
        return send(acc.at[1, 3, oy, c], r3.at[1], s3s.at[1], s3r.at[1], y_dev)

    def s3_het():
        return send(acc.at[2, 1, y, c], r3.at[2], s3s.at[2], s3r.at[2], a_dev)

    def s1_recv(p, i, t):
        for h in range(len(parts(i))):
            with jax.named_scope(f"s1_{p}"):
                s1(p, i, t, h).wait_recv()

    def add_allelic(tile, k):
        for t in range(2):
            s1_recv(1, k, t)
            acc[1, tile, t, c] = acc[1, tile, t, c] + r1[1, 2 * k + t]

    def add_het(tile, k):
        for t in range(2):
            s1_recv(2, k, t)
            acc[2, tile, t, c] = acc[2, tile, t, c] + r1[2, k + t]

    def add_total(k):
        s1_recv(0, k, 0)
        acc[0, k, y, c] = acc[0, k, y, c] + r1[0, k]

    def words_of(i):
        with jax.named_scope("words"):
            unpack_words(i)

    def turn_of(i):
        with jax.named_scope("turn"):
            turn(i)

    words_of(0)
    turn_of(0)
    matmul(0, 0, 0)
    matmul(1, 0, 0)
    marg_finish(0)
    marg_copy(1).start()
    matmul(2, 0, 0)
    s0_finish(0, 0, 0)
    matmul(0, 0, 1)
    s0_finish(1, 0, 0)
    marg_finish(1)
    marg_copy(2).start()
    matmul(1, 0, 1)
    s0_finish(2, 0, 0)
    matmul(2, 0, 1)
    s0_finish(0, 0, 1)
    words_of(1)
    s0_finish(1, 0, 1)
    turn_of(1)
    s0_finish(2, 0, 1)
    matmul(0, 1)
    matmul(1, 1)
    s0_finish(0, 1)
    words_of(2)
    s0_finish(1, 1)
    turn_of(2)
    marg_finish(2)
    marg_copy(3).start()
    matmul(2, 2)
    matmul(0, 2)
    s0_finish(2, 2)
    words_of(3)
    s0_finish(0, 2)
    turn_of(3)
    matmul(0, 3)
    matmul(1, 2)
    s0_finish(0, 3)
    matmul(2, 1)
    s0_finish(1, 2)
    add_allelic(2, 0)
    s2_allelic(0).start()
    s2_allelic(1).start()
    matmul(1, 3)
    s0_finish(2, 1)
    add_het(1, 0)
    s2_het(0).start()
    add_total(0)
    s2_total(0).start()
    matmul(2, 3)
    s0_finish(1, 3)
    add_total(1)
    s2_total(1).start()
    s0_finish(2, 3)
    add_allelic(3, 1)
    add_total(2)
    add_het(3, 2)
    s2_het(1).start()
    with jax.named_scope("s2_total"):
        s2_total(0).wait_recv()
    acc[0, 2, y, c] = acc[0, 2, y, c] + r2[0, 0]
    s3_total().start()
    with jax.named_scope("s2_allelic"):
        s2_allelic(0).wait_recv()
    acc[1, 3, oy, c] = acc[1, 3, oy, c] + r2[1, 0]
    s3_allelic().start()
    add_total(3)
    with jax.named_scope("s2_het"):
        s2_het(0).wait_recv()
    acc[2, 1, y, c] = acc[2, 1, y, c] + r2[2, 0]
    s3_het().start()

    marg_finish(3)
    gene_sum = marg[4, 0:1, :]
    gene_sq = marg[4, 1:2, :]
    lane = lax.broadcasted_iota(jnp.int32, (rows, marg.shape[2]), 1)
    row = lax.broadcasted_iota(jnp.int32, (rows, marg.shape[2]), 0)
    mine = lane == row + rows * s
    dos_sum = jnp.sum(jnp.where(mine, marg[4, 2:3, :], 0.0), axis=1, keepdims=True)
    dos_sq = jnp.sum(jnp.where(mine, marg[4, 3:4, :], 0.0), axis=1, keepdims=True)
    n = sample_count
    dosage_var = dos_sq - dos_sum * dos_sum / n
    gene_var = gene_sq - gene_sum * gene_sum / n

    with jax.named_scope("s2_allelic"):
        s2_allelic(1).wait_recv()
    with jax.named_scope("s2_het"):
        s2_het(1).wait_recv()
    with jax.named_scope("s2_total"):
        s2_total(1).wait_recv()
    with jax.named_scope("s3_allelic"):
        s3_allelic().wait_recv()
    with jax.named_scope("s3_het"):
        s3_het().wait_recv()
    allelic = acc[1, 3, y, c] + r2[1, 1] + r3[1]
    het_weight = acc[2, 3, y, c] + r2[2, 1] + r3[2]
    za_ref[...] = allelic / jnp.sqrt(het_weight + 1.0)
    with jax.named_scope("s3_total"):
        s3_total().wait_recv()
    total = acc[0, 3, y, c] + r2[0, 1] + r3[0]
    covariance = total - dos_sum * (gene_sum / n)
    scale = jnp.sqrt((dosage_var + 1.0) * (gene_var + 1.0))
    zt_ref[...] = (n**0.5) * covariance / scale

    for k in range(1, n_var):
        hap_copy(k).wait_send()
    for k in range(4):
        marg_copy(k).wait_send()

    for i in range(4):
        for p in range(3):
            for h in range(len(parts(i))):
                for t in range(2):
                    s0(p, i, t, h).wait_send()
                for t in s1_pieces(p, i):
                    s1(p, i, t, h).wait_send()
    for i in range(2):
        s2_total(i).wait_send()
        s2_allelic(i).wait_send()
        s2_het(i).wait_send()
    s3_total().wait_send()
    s3_allelic().wait_send()
    s3_het().wait_send()


def per_device(sample_count, hap_words, total_counts, allele_one, allele_two):
    n_var = lax.axis_size("var")
    words, block = hap_words.shape[1:]
    samples, genes = total_counts.shape
    variants = block * n_var
    rows = variants // 16
    tile = variants // 4
    dma = pltpu.SemaphoreType.DMA
    out = jax.ShapeDtypeStruct((rows, genes), F32)
    return pl.pallas_call(
        functools.partial(kernel, n_var, float(sample_count)),
        out_shape=(out, out),
        in_specs=[pl.BlockSpec(memory_space=pltpu.HBM)] * 4,
        out_specs=(pl.BlockSpec(memory_space=pltpu.VMEM),) * 2,
        scratch_shapes=[
            pltpu.VMEM((n_var, 2, words, block), jnp.int32),
            pltpu.VMEM((3, samples, genes), BF16),
            pltpu.VMEM((SLOTS, 3, ROWS_IN, genes), jnp.int32),
            pltpu.VMEM((2, 8, genes), F32),
            pltpu.VMEM((2, samples, 128), BF16),
            pltpu.VMEM((4, 3, tile, samples), BF16),
            pltpu.VMEM((3, 4, 2, 2, rows, genes), F32),
            pltpu.VMEM((3, 4, 2, rows, genes), F32),
            pltpu.VMEM((3, 4, rows, genes), F32),
            pltpu.VMEM((3, 2, rows, genes), F32),
            pltpu.VMEM((3, rows, genes), F32),
            pltpu.VMEM((5, 8, variants), F32),
            pltpu.VMEM((4, 8, variants), F32),
            dma((SLOTS, 3)),
            dma,
            dma((n_var,)),
            dma((n_var,)),
            dma((3, 4, 2, 2)),
            dma((3, 4, 2, 2)),
            dma((3, 4, 2)),
            dma((3, 4, 2)),
            dma((3, 2)),
            dma((3, 2)),
            dma((3,)),
            dma((3,)),
            dma((4,)),
            dma((4,)),
        ],
        compiler_params=pltpu.CompilerParams(
            collective_id=0,
            has_side_effects=True,
            vmem_limit_bytes=55_600_000,
        ),
    )(hap_words, total_counts, allele_one, allele_two)


def solution(mesh):
    in_specs = (P(None, "samp", "var"), P("samp", "var"), P("samp", "var"), P("samp", "var"))
    out_specs = (P("samp", "var"), P("samp", "var"))

    def whole(hap_words, total_counts, allele_one, allele_two):
        body = functools.partial(per_device, total_counts.shape[0])
        return jax.shard_map(
            body, mesh=mesh, in_specs=in_specs, out_specs=out_specs, check_vma=False
        )(hap_words, total_counts, allele_one, allele_two)

    return whole
```

```python
import functools

import jax
import jax.numpy as jnp
from jax import lax
from jax.experimental import pallas as pl
from jax.experimental.pallas import tpu as pltpu
from jax.sharding import PartitionSpec as P

BITS = 30
ROWS_IN = 128
SLOTS = 6
TURN = 5
DEFER = 2
STEP = 16
SEND_AT = (0, 4, 8, 12)
FAR_FIRST = (5, 4, 7, 6, 1, 3, 2)
LANES = 256
MESH = pl.DeviceIdType.MESH
BF16 = jnp.bfloat16
F32 = jnp.float32


def kernel(
    n_var,
    sample_count,
    hap_ref,
    total_ref,
    one_ref,
    two_ref,
    zt_ref,
    za_ref,
    hall,
    feats,
    gacc,
    acc,
    r0,
    r1,
    r2,
    r3,
    marg,
    mrecv,
    in_sem,
    hap_own,
    hap_send,
    hap_recv,
    s0s,
    s0r,
    s1s,
    s1r,
    s2s,
    s2r,
    s3s,
    s3r,
    ms,
    mr,
):
    samples, genes = total_ref.shape
    words = hap_ref.shape[1]
    rows = acc.shape[4]
    s = lax.axis_index("samp")
    v = lax.axis_index("var")
    c = s % 2
    y = (s // 2) % 2
    z = s // 4
    x = v // 2
    za = z + 1 - 2 * (z % 2)
    zb = 3 - z
    zc = (z + 2) % 4
    core_dev = (s + 1 - 2 * c, v)
    y_dev = (s + 2 - 4 * y, v)
    a_dev = (za * 4 + y * 2 + c, v)
    b_dev = (zb * 4 + y * 2 + c, v)
    chips = [((s + 2 * j) % 16, v) for j in range(1, 8)]
    oc = 1 - c
    oy = 1 - y

    half = genes // 2
    halves = (pl.ds(0, half), pl.ds(half, half))
    quarter = half // 2
    early = (pl.ds(0, quarter), pl.ds(quarter, quarter), halves[1])

    def pieces(i):
        return early if i == 0 else halves

    def pieces_of_half(i, h):
        return ((0, 1), (2,))[h] if i == 0 else (h,)

    n_chunks = samples // ROWS_IN

    def fetch(counts, k, slot, which, ref):
        at = pl.multiple_of(k * ROWS_IN, ROWS_IN)
        return pltpu.make_async_copy(
            ref.at[pl.ds(at, ROWS_IN), :],
            counts.at[slot, which],
            in_sem.at[slot],
        )

    sources = (total_ref, one_ref, two_ref)
    own = pltpu.make_async_copy(hap_ref, hall.at[v], hap_own)

    def peer(k, sign):
        return ((x + sign * (k // 2) + 4) % 4) * 2 + (v + k) % 2

    def hap_copy(k):
        return pltpu.make_async_remote_copy(
            src_ref=hap_ref,
            dst_ref=hall.at[v],
            send_sem=hap_send,
            recv_sem=hap_recv.at[k],
            device_id=(s, peer(k, 1)),
            device_id_type=MESH,
        )

    def hap_arrival(k):
        return pltpu.make_async_remote_copy(
            src_ref=hap_ref,
            dst_ref=hall.at[peer(k, -1)],
            send_sem=hap_send,
            recv_sem=hap_recv.at[k],
            device_id=(s, peer(k, 1)),
            device_id_type=MESH,
        )

    at_tile = [jnp.where(x == w, k, 0) for w, k in zip((zc, za, zb, z), SEND_AT)]
    send_at = sum(at_tile)

    gacc[...] = jnp.zeros_like(gacc)

    def chunk_step(counts, k, carry):
        slot = k % SLOTS

        @pl.when(k == send_at)
        def _():
            for m in FAR_FIRST:
                hap_copy(m).start()

        @pl.when(k + SLOTS - 1 < n_chunks)
        def _():
            for which, ref in enumerate(sources):
                fetch(counts, k + SLOTS - 1, (k + SLOTS - 1) % SLOTS, which, ref).start()

        pltpu.make_async_copy(counts.at[slot], counts.at[slot], in_sem.at[slot]).wait()
        def row_step(r, carry):
            at = pl.ds(pl.multiple_of(r * STEP, STEP), STEP)
            out = pl.ds(pl.multiple_of(k * ROWS_IN + r * STEP, STEP), STEP)
            for lane in range(0, genes, LANES):
                cols = pl.ds(lane, LANES)
                log_total = jnp.log((counts[slot, 0, at, cols] + 1).astype(F32))
                one = (counts[slot, 1, at, cols] + 1).astype(F32)
                two = (counts[slot, 2, at, cols] + 1).astype(F32)
                weight = (one * two) / (one + two)
                weighted = weight * (jnp.log(one) - jnp.log(two))
                feats[0, out, cols] = log_total.astype(BF16)
                feats[1, out, cols] = weighted.astype(BF16)
                feats[2, out, cols] = weight.astype(BF16)
                square = log_total * log_total
                gacc[0, :, cols] += log_total[:8] + log_total[8:]
                gacc[1, :, cols] += square[:8] + square[8:]
            return carry

        lax.fori_loop(0, ROWS_IN // STEP, row_step, 0, unroll=2)
        return carry

    def features(counts):
        for k in range(SLOTS - 1):
            for which, ref in enumerate(sources):
                fetch(counts, k, k, which, ref).start()

        barrier = pltpu.get_barrier_semaphore()
        for dev in (core_dev, *chips):
            pl.semaphore_signal(barrier, inc=1, device_id=dev, device_id_type=MESH)
        for k in range(1, n_var):
            pl.semaphore_signal(
                barrier, inc=1, device_id=(s, (v + k) % n_var), device_id_type=MESH
            )
        own.start()
        with jax.named_scope("barrier"):
            pl.semaphore_wait(barrier, 8 + n_var - 1)
        step = functools.partial(chunk_step, counts)
        with jax.named_scope("features"):
            lax.fori_loop(0, n_chunks, step, 0)

    def hap_wait(i):
        target = (zc, za, zb, z)[i]
        with jax.named_scope("hap_wait"):
            for b in range(2):
                k = ((x + 4 - target) % 4) * 2 + (v + b) % 2

                @pl.when(k == 0)
                def _():
                    own.wait()

                @pl.when(k != 0)
                def _():
                    hap_arrival(k).wait_recv()

    def gene_margins():
        marg[0, 0, 0:1, :] = jnp.sum(gacc[0], axis=0, keepdims=True)
        marg[0, 0, 1:2, :] = jnp.sum(gacc[1], axis=0, keepdims=True)

    def variant_margins():
        for b in range(n_var):
            w0, w1 = hall[b, 0], hall[b, 1]
            bits = lax.population_count(w0) + lax.population_count(w1)
            het = lax.population_count(jnp.bitwise_xor(w0, w1))
            cols = pl.ds(b * 128, 128)
            bit_sum = jnp.sum(bits.astype(F32), axis=0, keepdims=True)
            het_sum = jnp.sum(het.astype(F32), axis=0, keepdims=True)
            marg[1, 0, 0:1, cols] = bit_sum - float(samples)
            marg[1, 0, 1:2, cols] = float(samples) - het_sum

    def marg_pair(w):
        return pltpu.make_async_remote_copy(
            src_ref=marg.at[w, 0],
            dst_ref=mrecv.at[w, 0],
            send_sem=ms,
            recv_sem=mr.at[w, 0],
            device_id=core_dev,
            device_id_type=MESH,
        )

    def marg_chip(w, j):
        return pltpu.make_async_remote_copy(
            src_ref=marg.at[w, 1],
            dst_ref=mrecv.at[w, j],
            send_sem=ms,
            recv_sem=mr.at[w, 1],
            device_id=chips[j - 1],
            device_id_type=MESH,
        )

    def marg_share(w):
        with jax.named_scope("marg_wait"):
            marg_pair(w).wait_recv()
        marg[w, 1] = marg[w, 0] + mrecv[w, 0]
        for j in range(1, 8):
            marg_chip(w, j).start()

    def marg_total(w):
        others = mrecv.at[w, pl.ds(1, 7)]
        with jax.named_scope("marg_wait"):
            pltpu.make_async_copy(others, others, mr.at[w, 1]).wait()
        total = marg[w, 1]
        for j in range(1, 8):
            total = total + mrecv[w, j]
        return total

    def send(src, dst, ss, rs, dev):
        return pltpu.make_async_remote_copy(
            src_ref=src,
            dst_ref=dst,
            send_sem=ss,
            recv_sem=rs,
            device_id=dev,
            device_id_type=MESH,
        )

    def at_piece(i, g):
        return g if i == 0 else 1 + 2 * i + g

    def s0(p, i, g):
        cols = pieces(i)[g]
        return send(
            acc.at[p, i, :, oc, :, cols],
            r0.at[p, i, :, :, cols],
            s0s,
            s0r.at[p, at_piece(i, g)],
            core_dev,
        )

    def s1(p, i, g):
        cols = pieces(i)[g]
        if p == 0:
            src, dst, dev = acc.at[p, i, oy, c, :, cols], r1.at[p, i, :, cols], y_dev
        else:
            dev = a_dev if p == 1 else b_dev
            first = 2 * i if p == 1 else i
            src, dst = acc.at[p, i, :, c, :, cols], r1.at[p, pl.ds(first, 2), :, cols]
        return send(src, dst, s1s, s1r.at[p, at_piece(i, g)], dev)

    def goes_on(p, i):
        return p == 0 or (i < 2 if p == 1 else i % 2 == 0)

    def s0_finish(p, i, g):
        cols = pieces(i)[g]
        with jax.named_scope("s0_wait"):
            s0(p, i, g).wait_recv()
        for t in range(2):
            acc[p, i, t, c, :, cols] += r0[p, i, t, :, cols]
        if goes_on(p, i):
            s1(p, i, g).start()

    iota = lax.broadcasted_iota(jnp.int32, (8, 128), 0)

    def unpack_words(tbuf, i):
        zt = (zc, za, zb, z)[i]
        for b in range(2):
            block = 2 * zt + b

            def word_step(g, carry):
                at = pl.ds(pl.multiple_of(g * 8, 8), 8)
                w0 = hall[block, 0, at, :]
                w1 = hall[block, 1, at, :] << 1
                parts = []
                for t in range(BITS):
                    first = 8 * t // BITS
                    last = (8 * t + 7) // BITS
                    shift = iota + (8 * t - BITS * first)
                    u0 = jnp.broadcast_to(w0[first : first + 1], (8, 128))
                    u1 = jnp.broadcast_to(w1[first : first + 1], (8, 128))
                    if last != first:
                        early = iota < BITS * last - 8 * t
                        shift = jnp.where(early, shift, shift - BITS)
                        u0 = jnp.where(early, u0, jnp.broadcast_to(w0[last : last + 1], (8, 128)))
                        u1 = jnp.where(early, u1, jnp.broadcast_to(w1[last : last + 1], (8, 128)))
                    code = ((u0 >> shift) & 1) | ((u1 >> shift) & 2)
                    parts.append(code.astype(F32))
                out = pl.ds(pl.multiple_of(g * 8 * BITS, 16), 8 * BITS)
                tbuf[b, out, :] = jnp.concatenate(parts, axis=0).astype(BF16)
                return carry

            lax.fori_loop(0, words // 8, word_step, 0)

    def turn(tbuf, lhs, i):
        def turn_step(k, carry):
            for b in range(2):
                for j in range(TURN):
                    at = pl.ds(pl.multiple_of(k * (TURN * 128) + j * 128, 128), 128)
                    centred = tbuf[b, at, :].T - 1.5
                    het = jnp.abs(centred) < 1.0
                    zero = jnp.zeros_like(centred)
                    out = pl.ds(b * 128, 128)
                    lhs[i, 0, out, at] = jnp.clip(jnp.where(het, zero, centred), -1.0, 1.0)
                    lhs[i, 1, out, at] = jnp.where(het, centred * -2.0, zero)
                    lhs[i, 2, out, at] = jnp.where(het, jnp.ones_like(centred), zero)
            return carry

        lax.fori_loop(0, samples // (TURN * 128), turn_step, 0)

    def matmul(lhs, p, i, h):
        cols = pieces(i)[h]
        with jax.named_scope("matmul"):
            res = jnp.dot(lhs[i, p], feats[p, :, cols], preferred_element_type=F32)
            acc[p, i, :, :, :, cols] = res.reshape(2, 2, rows, res.shape[1])
        s0(p, i, h).start()

    def s2(p, k, h):
        if p == 0:
            src, dev = (k, y), a_dev
        elif p == 1:
            src, dev = (2, oy if k == 0 else y), b_dev
        else:
            src, dev = (1 + 2 * k, oy), y_dev
        return send(
            acc.at[p, src[0], src[1], c, :, halves[h]],
            r2.at[p, k, :, halves[h]],
            s2s,
            s2r.at[p, k, h],
            dev,
        )

    def s3(p, h):
        src, dev = (((2, y), b_dev), ((3, oy), y_dev), ((1, y), a_dev))[p]
        return send(
            acc.at[p, src[0], src[1], c, :, halves[h]],
            r3.at[p, :, halves[h]],
            s3s,
            s3r.at[p, h],
            dev,
        )

    def s1_arrival(p, i, h):
        for g in pieces_of_half(i, h):
            with jax.named_scope(f"s1_{p}"):
                s1(p, i, g).wait_recv()

    def add_allelic(tile, k, h):
        s1_arrival(1, k, h)
        for t in range(2):
            acc[1, tile, t, c, :, halves[h]] += r1[1, 2 * k + t, :, halves[h]]

    def add_het(tile, k, h):
        s1_arrival(2, k, h)
        for t in range(2):
            acc[2, tile, t, c, :, halves[h]] += r1[2, k + t, :, halves[h]]

    def add_total(k, h):
        s1_arrival(0, k, h)
        acc[0, k, y, c, :, halves[h]] += r1[0, k, :, halves[h]]

    def pass_on(p, h):
        with jax.named_scope(f"s2_{p}_0"):
            s2(p, 0, h).wait_recv()
        tile, t = ((2, y), (3, oy), (1, y))[p]
        acc[p, tile, t, c, :, halves[h]] += r2[p, 0, :, halves[h]]
        s3(p, h).start()

    def last_add(p, h):
        with jax.named_scope(f"s2_{p}_1"):
            s2(p, 1, h).wait_recv()
        with jax.named_scope(f"s3_{p}"):
            s3(p, h).wait_recv()
        return acc[p, 3, y, c, :, halves[h]] + r2[p, 1, :, halves[h]] + r3[p, :, halves[h]]

    def all_sent(ref, sem):
        pltpu.make_async_copy(ref, ref, sem).wait()

    def drain_first():
        all_sent(hall.at[pl.ds(0, n_var - 1)], hap_send)
        all_sent(mrecv, ms)
        all_sent(r0, s0s)
        all_sent(r1, s1s)

    def products(tbuf, lhs):
        def words_of(i):
            hap_wait(i)
            with jax.named_scope("words"):
                unpack_words(tbuf, i)

        def turn_of(i):
            with jax.named_scope("turn"):
                turn(tbuf, lhs, i)

        pending = []

        def mm(*steps):
            for step in steps:
                matmul(lhs, *step)
                pending.append(step)
                if len(pending) > (DEFER if step[1] else DEFER + 1):
                    go_on(1)

        def go_on(count):
            for step in pending[:count]:
                s0_finish(*step)
            del pending[:count]

        words_of(0)
        marg_share(0)
        turn_of(0)
        for g in range(3):
            mm((0, 0, g), (1, 0, g), (2, 0, g))
        words_of(1)
        go_on(3)
        turn_of(1)
        mm((0, 1, 0), (0, 1, 1))
        words_of(2)
        go_on(2)
        turn_of(2)
        mm((0, 2, 0), (1, 1, 0), (2, 2, 0), (0, 2, 1))
        words_of(3)
        go_on(2)
        turn_of(3)
        variant_margins()
        marg_pair(1).start()
        mm((0, 3, 0), (1, 1, 1), (2, 2, 1), (0, 3, 1))
        marg_share(1)
        mm((1, 2, 0), (2, 1, 0), (1, 2, 1), (2, 1, 1))
        add_allelic(2, 0, 0)
        s2(1, 0, 0).start()
        add_total(0, 0)
        s2(0, 0, 0).start()
        mm((2, 3, 0),)
        add_het(1, 0, 0)
        s2(2, 0, 0).start()
        add_total(0, 1)
        s2(0, 0, 1).start()
        mm((1, 3, 0))
        add_allelic(2, 0, 1)
        for k, h in ((0, 1), (1, 0), (1, 1)):
            s2(1, k, h).start()
        mm((2, 3, 1))
        add_het(1, 0, 1)
        s2(2, 0, 1).start()
        mm((1, 3, 1))
        go_on(len(pending))

    variants = n_var * 128
    pl.run_scoped(features, pltpu.VMEM((SLOTS, 3, ROWS_IN, genes), jnp.int32))
    gene_margins()
    marg_pair(0).start()
    pl.run_scoped(
        products,
        pltpu.VMEM((2, samples, 128), BF16),
        pltpu.VMEM((4, 3, variants // 4, samples), BF16),
    )
    for h in range(2):
        add_total(1, h)
        s2(0, 1, h).start()
    add_het(3, 2, 0)
    s2(2, 1, 0).start()
    add_allelic(3, 1, 0)
    add_total(2, 0)
    add_total(2, 1)
    add_allelic(3, 1, 1)
    add_total(3, 0)
    add_het(3, 2, 1)
    s2(2, 1, 1).start()
    add_total(3, 1)
    for p in (2, 0, 1):
        pass_on(p, 0)
    for p in (2, 0, 1):
        pass_on(p, 1)

    gene_total = marg_total(0)
    variant_total = marg_total(1)
    gene_sum = gene_total[0:1]
    gene_sq = gene_total[1:2]
    lane = lax.broadcasted_iota(jnp.int32, (rows, marg.shape[3]), 1)
    row = lax.broadcasted_iota(jnp.int32, (rows, marg.shape[3]), 0)
    mine = lane == row + rows * s
    dos_sum = jnp.sum(jnp.where(mine, variant_total[0:1], 0.0), axis=1, keepdims=True)
    dos_sq = jnp.sum(jnp.where(mine, variant_total[1:2], 0.0), axis=1, keepdims=True)
    n = sample_count
    dosage_var = dos_sq - dos_sum * dos_sum / n
    gene_var = gene_sq - gene_sum * gene_sum / n
    with jax.named_scope("drain_first"):
        drain_first()
    mean = gene_sum / n
    scale = (n**0.5) / jnp.sqrt((dosage_var + 1.0) * (gene_var + 1.0))
    for h in range(2):
        cols = halves[h]
        allelic = last_add(1, h)
        het_weight = last_add(2, h)
        with jax.named_scope("fin_a"):
            za_ref[:, cols] = allelic / jnp.sqrt(het_weight + 1.0)
        if h == 1:
            all_sent(r2, s2s)
        total = last_add(0, h)
        at = slice(h * half, (h + 1) * half)
        with jax.named_scope("fin_t"):
            zt_ref[:, cols] = (total - dos_sum * mean[:, at]) * scale[:, at]

    with jax.named_scope("drain"):
        all_sent(r3, s3s)


def per_device(sample_count, hap_words, total_counts, allele_one, allele_two):
    n_var = lax.axis_size("var")
    words, block = hap_words.shape[1:]
    samples, genes = total_counts.shape
    variants = block * n_var
    rows = variants // 16
    dma = pltpu.SemaphoreType.DMA
    out = jax.ShapeDtypeStruct((rows, genes), F32)
    return pl.pallas_call(
        functools.partial(kernel, n_var, float(sample_count)),
        out_shape=(out, out),
        in_specs=[pl.BlockSpec(memory_space=pltpu.HBM)] * 4,
        out_specs=(pl.BlockSpec(memory_space=pltpu.VMEM),) * 2,
        scratch_shapes=[
            pltpu.VMEM((n_var, 2, words, block), jnp.int32),
            pltpu.VMEM((3, samples, genes), BF16),
            pltpu.VMEM((2, 8, genes), F32),
            pltpu.VMEM((3, 4, 2, 2, rows, genes), F32),
            pltpu.VMEM((3, 4, 2, rows, genes), F32),
            pltpu.VMEM((3, 4, rows, genes), F32),
            pltpu.VMEM((3, 2, rows, genes), F32),
            pltpu.VMEM((3, rows, genes), F32),
            pltpu.VMEM((2, 2, 2, variants), F32),
            pltpu.VMEM((2, 8, 2, variants), F32),
            dma((SLOTS,)),
            dma,
            dma,
            dma((n_var,)),
            dma,
            dma((3, 9)),
            dma,
            dma((3, 9)),
            dma,
            dma((3, 2, 2)),
            dma,
            dma((3, 2)),
            dma,
            dma((2, 2)),
        ],
        compiler_params=pltpu.CompilerParams(
            collective_id=0,
            has_side_effects=True,
            vmem_limit_bytes=55_600_000,
        ),
    )(hap_words, total_counts, allele_one, allele_two)


def solution(mesh):
    in_specs = (P(None, "samp", "var"), P("samp", "var"), P("samp", "var"), P("samp", "var"))
    out_specs = (P("samp", "var"), P("samp", "var"))

    def whole(hap_words, total_counts, allele_one, allele_two):
        body = functools.partial(per_device, total_counts.shape[0])
        return jax.shard_map(
            body, mesh=mesh, in_specs=in_specs, out_specs=out_specs, check_vma=False
        )(hap_words, total_counts, allele_one, allele_two)

    return whole
```

```python
import functools

import jax
import jax.numpy as jnp
from jax import lax
from jax.experimental import pallas as pl
from jax.experimental.pallas import tpu as pltpu
from jax.sharding import PartitionSpec as P

BITS = 30
ROWS_IN = 128
SLOTS = 6
TURN = 5
DEFER = 2
STEP = 16
SEND_AT = (0, 4, 8, 12)
FAR_FIRST = (5, 4, 7, 6, 1, 3, 2)
LANES = 256
MESH = pl.DeviceIdType.MESH
BF16 = jnp.bfloat16
F32 = jnp.float32


def kernel(
    n_var,
    sample_count,
    hap_ref,
    total_ref,
    one_ref,
    two_ref,
    zt_ref,
    za_ref,
    hall,
    feats,
    gacc,
    acc,
    r0,
    r1,
    r2,
    r3,
    marg,
    mrecv,
    in_sem,
    hap_own,
    hap_send,
    hap_recv,
    s0s,
    s0r,
    s1s,
    s1r,
    s2s,
    s2r,
    s3s,
    s3r,
    ms,
    mr,
):
    samples, genes = total_ref.shape
    words = hap_ref.shape[1]
    rows = acc.shape[4]
    s = lax.axis_index("samp")
    v = lax.axis_index("var")
    c = s % 2
    y = (s // 2) % 2
    z = s // 4
    x = v // 2
    za = z + 1 - 2 * (z % 2)
    zb = 3 - z
    zc = (z + 2) % 4
    core_dev = (s + 1 - 2 * c, v)
    y_dev = (s + 2 - 4 * y, v)
    a_dev = (za * 4 + y * 2 + c, v)
    b_dev = (zb * 4 + y * 2 + c, v)
    chips = [((s + 2 * j) % 16, v) for j in range(1, 8)]
    oc = 1 - c
    oy = 1 - y

    half = genes // 2
    halves = (pl.ds(0, half), pl.ds(half, half))

    n_chunks = samples // ROWS_IN

    def fetch(counts, k, slot, which, ref):
        at = pl.multiple_of(k * ROWS_IN, ROWS_IN)
        return pltpu.make_async_copy(
            ref.at[pl.ds(at, ROWS_IN), :],
            counts.at[slot, which],
            in_sem.at[slot],
        )

    sources = (total_ref, one_ref, two_ref)
    own = pltpu.make_async_copy(hap_ref, hall.at[v], hap_own)

    def peer(k, sign):
        return ((x + sign * (k // 2) + 4) % 4) * 2 + (v + k) % 2

    def hap_copy(k):
        return pltpu.make_async_remote_copy(
            src_ref=hap_ref,
            dst_ref=hall.at[v],
            send_sem=hap_send,
            recv_sem=hap_recv.at[k],
            device_id=(s, peer(k, 1)),
            device_id_type=MESH,
        )

    def hap_arrival(k):
        return pltpu.make_async_remote_copy(
            src_ref=hap_ref,
            dst_ref=hall.at[peer(k, -1)],
            send_sem=hap_send,
            recv_sem=hap_recv.at[k],
            device_id=(s, peer(k, 1)),
            device_id_type=MESH,
        )

    at_tile = [jnp.where(x == w, k, 0) for w, k in zip((zc, za, zb, z), SEND_AT)]
    send_at = sum(at_tile)

    gacc[...] = jnp.zeros_like(gacc)

    def chunk_step(counts, k, carry):
        slot = k % SLOTS

        @pl.when(k == send_at)
        def _():
            for m in FAR_FIRST:
                hap_copy(m).start()

        @pl.when(k + SLOTS - 1 < n_chunks)
        def _():
            for which, ref in enumerate(sources):
                fetch(counts, k + SLOTS - 1, (k + SLOTS - 1) % SLOTS, which, ref).start()

        pltpu.make_async_copy(counts.at[slot], counts.at[slot], in_sem.at[slot]).wait()
        def row_step(r, carry):
            at = pl.ds(pl.multiple_of(r * STEP, STEP), STEP)
            out = pl.ds(pl.multiple_of(k * ROWS_IN + r * STEP, STEP), STEP)
            for lane in range(0, genes, LANES):
                cols = pl.ds(lane, LANES)
                log_total = jnp.log((counts[slot, 0, at, cols] + 1).astype(F32))
                one = (counts[slot, 1, at, cols] + 1).astype(F32)
                two = (counts[slot, 2, at, cols] + 1).astype(F32)
                weight = (one * two) / (one + two)
                weighted = weight * (jnp.log(one) - jnp.log(two))
                feats[0, out, cols] = log_total.astype(BF16)
                feats[1, out, cols] = weighted.astype(BF16)
                feats[2, out, cols] = weight.astype(BF16)
                square = log_total * log_total
                gacc[0, :, cols] += log_total[:8] + log_total[8:]
                gacc[1, :, cols] += square[:8] + square[8:]
            return carry

        lax.fori_loop(0, ROWS_IN // STEP, row_step, 0, unroll=2)
        return carry

    def features(counts):
        for k in range(SLOTS - 1):
            for which, ref in enumerate(sources):
                fetch(counts, k, k, which, ref).start()

        barrier = pltpu.get_barrier_semaphore()
        for dev in (core_dev, *chips):
            pl.semaphore_signal(barrier, inc=1, device_id=dev, device_id_type=MESH)
        for k in range(1, n_var):
            pl.semaphore_signal(
                barrier, inc=1, device_id=(s, (v + k) % n_var), device_id_type=MESH
            )
        own.start()
        with jax.named_scope("barrier"):
            pl.semaphore_wait(barrier, 8 + n_var - 1)
        step = functools.partial(chunk_step, counts)
        with jax.named_scope("features"):
            lax.fori_loop(0, n_chunks, step, 0)

    def hap_wait(i):
        target = (zc, za, zb, z)[i]
        with jax.named_scope("hap_wait"):
            for b in range(2):
                k = ((x + 4 - target) % 4) * 2 + (v + b) % 2

                @pl.when(k == 0)
                def _():
                    own.wait()

                @pl.when(k != 0)
                def _():
                    hap_arrival(k).wait_recv()

    def gene_margins():
        marg[0, 0, 0:1, :] = jnp.sum(gacc[0], axis=0, keepdims=True)
        marg[0, 0, 1:2, :] = jnp.sum(gacc[1], axis=0, keepdims=True)

    def variant_margins():
        for b in range(n_var):
            w0, w1 = hall[b, 0], hall[b, 1]
            bits = lax.population_count(w0) + lax.population_count(w1)
            het = lax.population_count(jnp.bitwise_xor(w0, w1))
            cols = pl.ds(b * 128, 128)
            bit_sum = jnp.sum(bits.astype(F32), axis=0, keepdims=True)
            het_sum = jnp.sum(het.astype(F32), axis=0, keepdims=True)
            marg[1, 0, 0:1, cols] = bit_sum - float(samples)
            marg[1, 0, 1:2, cols] = float(samples) - het_sum

    def marg_pair(w):
        return pltpu.make_async_remote_copy(
            src_ref=marg.at[w, 0],
            dst_ref=mrecv.at[w, 0],
            send_sem=ms,
            recv_sem=mr.at[w, 0],
            device_id=core_dev,
            device_id_type=MESH,
        )

    def marg_chip(w, j):
        return pltpu.make_async_remote_copy(
            src_ref=marg.at[w, 1],
            dst_ref=mrecv.at[w, j],
            send_sem=ms,
            recv_sem=mr.at[w, 1],
            device_id=chips[j - 1],
            device_id_type=MESH,
        )

    def marg_share(w):
        with jax.named_scope("marg_wait"):
            marg_pair(w).wait_recv()
        marg[w, 1] = marg[w, 0] + mrecv[w, 0]
        for j in range(1, 8):
            marg_chip(w, j).start()

    def marg_total(w):
        others = mrecv.at[w, pl.ds(1, 7)]
        with jax.named_scope("marg_wait"):
            pltpu.make_async_copy(others, others, mr.at[w, 1]).wait()
        total = marg[w, 1]
        for j in range(1, 8):
            total = total + mrecv[w, j]
        return total

    def send(src, dst, ss, rs, dev):
        return pltpu.make_async_remote_copy(
            src_ref=src,
            dst_ref=dst,
            send_sem=ss,
            recv_sem=rs,
            device_id=dev,
            device_id_type=MESH,
        )

    def s0(p, i, g):
        cols = halves[g]
        return send(
            acc.at[p, i, :, oc, :, cols],
            r0.at[p, i, :, :, cols],
            s0s,
            s0r.at[p, 2 * i + g],
            core_dev,
        )

    def s1(p, i, g):
        cols = halves[g]
        if p == 0:
            src, dst, dev = acc.at[p, i, oy, c, :, cols], r1.at[p, i, :, cols], y_dev
        else:
            dev = a_dev if p == 1 else b_dev
            first = 2 * i if p == 1 else i
            src, dst = acc.at[p, i, :, c, :, cols], r1.at[p, pl.ds(first, 2), :, cols]
        return send(src, dst, s1s, s1r.at[p, 2 * i + g], dev)

    def goes_on(p, i):
        return p == 0 or (i < 2 if p == 1 else i % 2 == 0)

    def s0_finish(p, i, g):
        cols = halves[g]
        with jax.named_scope("s0_wait"):
            s0(p, i, g).wait_recv()
        for t in range(2):
            acc[p, i, t, c, :, cols] += r0[p, i, t, :, cols]
        if goes_on(p, i):
            s1(p, i, g).start()

    iota = lax.broadcasted_iota(jnp.int32, (8, 128), 0)

    def unpack_words(tbuf, i):
        zt = (zc, za, zb, z)[i]
        for b in range(2):
            block = 2 * zt + b

            def word_step(g, carry):
                at = pl.ds(pl.multiple_of(g * 8, 8), 8)
                w0 = hall[block, 0, at, :]
                w1 = hall[block, 1, at, :] << 1
                parts = []
                for t in range(BITS):
                    first = 8 * t // BITS
                    last = (8 * t + 7) // BITS
                    shift = iota + (8 * t - BITS * first)
                    u0 = jnp.broadcast_to(w0[first : first + 1], (8, 128))
                    u1 = jnp.broadcast_to(w1[first : first + 1], (8, 128))
                    if last != first:
                        early = iota < BITS * last - 8 * t
                        shift = jnp.where(early, shift, shift - BITS)
                        u0 = jnp.where(early, u0, jnp.broadcast_to(w0[last : last + 1], (8, 128)))
                        u1 = jnp.where(early, u1, jnp.broadcast_to(w1[last : last + 1], (8, 128)))
                    code = ((u0 >> shift) & 1) | ((u1 >> shift) & 2)
                    parts.append(code.astype(F32))
                out = pl.ds(pl.multiple_of(g * 8 * BITS, 16), 8 * BITS)
                tbuf[b, out, :] = jnp.concatenate(parts, axis=0).astype(BF16)
                return carry

            lax.fori_loop(0, words // 8, word_step, 0)

    def turn(tbuf, lhs, i):
        def turn_step(k, carry):
            for b in range(2):
                for j in range(TURN):
                    at = pl.ds(pl.multiple_of(k * (TURN * 128) + j * 128, 128), 128)
                    centred = tbuf[b, at, :].T - 1.5
                    het = jnp.abs(centred) < 1.0
                    zero = jnp.zeros_like(centred)
                    out = pl.ds(b * 128, 128)
                    lhs[i, 0, out, at] = jnp.clip(jnp.where(het, zero, centred), -1.0, 1.0)
                    lhs[i, 1, out, at] = jnp.where(het, centred * -2.0, zero)
                    lhs[i, 2, out, at] = jnp.where(het, jnp.ones_like(centred), zero)
            return carry

        lax.fori_loop(0, samples // (TURN * 128), turn_step, 0)

    def matmul(lhs, p, i, h):
        cols = halves[h]
        with jax.named_scope("matmul"):
            res = jnp.dot(lhs[i, p], feats[p, :, cols], preferred_element_type=F32)
            acc[p, i, :, :, :, cols] = res.reshape(2, 2, rows, res.shape[1])
        s0(p, i, h).start()

    def s2(p, k, h):
        if p == 0:
            src, dev = (k, y), a_dev
        elif p == 1:
            src, dev = (2, oy if k == 0 else y), b_dev
        else:
            src, dev = (1 + 2 * k, oy), y_dev
        return send(
            acc.at[p, src[0], src[1], c, :, halves[h]],
            r2.at[p, k, :, halves[h]],
            s2s,
            s2r.at[p, k, h],
            dev,
        )

    def s3(p, h):
        src, dev = (((2, y), b_dev), ((3, oy), y_dev), ((1, y), a_dev))[p]
        return send(
            acc.at[p, src[0], src[1], c, :, halves[h]],
            r3.at[p, :, halves[h]],
            s3s,
            s3r.at[p, h],
            dev,
        )

    def s1_arrival(p, i, h):
        with jax.named_scope(f"s1_{p}"):
            s1(p, i, h).wait_recv()

    def add_allelic(tile, k, h):
        s1_arrival(1, k, h)
        for t in range(2):
            acc[1, tile, t, c, :, halves[h]] += r1[1, 2 * k + t, :, halves[h]]

    def add_het(tile, k, h):
        s1_arrival(2, k, h)
        for t in range(2):
            acc[2, tile, t, c, :, halves[h]] += r1[2, k + t, :, halves[h]]

    def add_total(k, h):
        s1_arrival(0, k, h)
        acc[0, k, y, c, :, halves[h]] += r1[0, k, :, halves[h]]

    def pass_on(p, h):
        with jax.named_scope(f"s2_{p}_0"):
            s2(p, 0, h).wait_recv()
        tile, t = ((2, y), (3, oy), (1, y))[p]
        acc[p, tile, t, c, :, halves[h]] += r2[p, 0, :, halves[h]]
        s3(p, h).start()

    def last_add(p, h):
        with jax.named_scope(f"s2_{p}_1"):
            s2(p, 1, h).wait_recv()
        with jax.named_scope(f"s3_{p}"):
            s3(p, h).wait_recv()
        return acc[p, 3, y, c, :, halves[h]] + r2[p, 1, :, halves[h]] + r3[p, :, halves[h]]

    def all_sent(ref, sem):
        pltpu.make_async_copy(ref, ref, sem).wait()

    def drain_first():
        all_sent(hall.at[pl.ds(0, n_var - 1)], hap_send)
        all_sent(mrecv, ms)
        all_sent(r0, s0s)
        all_sent(r1, s1s)

    def products(tbuf, lhs):
        def words_of(i):
            hap_wait(i)
            with jax.named_scope("words"):
                unpack_words(tbuf, i)

        def turn_of(i):
            with jax.named_scope("turn"):
                turn(tbuf, lhs, i)

        pending = []

        def mm(*steps):
            for step in steps:
                matmul(lhs, *step)
                pending.append(step)
                if len(pending) > DEFER:
                    go_on(1)

        def go_on(count):
            for step in pending[:count]:
                s0_finish(*step)
            del pending[:count]

        words_of(0)
        marg_share(0)
        turn_of(0)
        for g in range(2):
            mm((0, 0, g), (1, 0, g), (2, 0, g))
        words_of(1)
        go_on(2)
        turn_of(1)
        mm((0, 1, 0), (0, 1, 1))
        words_of(2)
        go_on(2)
        turn_of(2)
        mm((0, 2, 0), (1, 1, 0), (2, 2, 0), (0, 2, 1))
        words_of(3)
        go_on(2)
        turn_of(3)
        variant_margins()
        marg_pair(1).start()
        mm((0, 3, 0), (1, 1, 1), (2, 2, 1), (0, 3, 1))
        marg_share(1)
        mm((1, 2, 0), (2, 1, 0), (1, 2, 1), (2, 1, 1))
        add_allelic(2, 0, 0)
        s2(1, 0, 0).start()
        add_total(0, 0)
        s2(0, 0, 0).start()
        mm((2, 3, 0),)
        add_het(1, 0, 0)
        s2(2, 0, 0).start()
        add_total(0, 1)
        s2(0, 0, 1).start()
        mm((1, 3, 0))
        add_allelic(2, 0, 1)
        for k, h in ((0, 1), (1, 0), (1, 1)):
            s2(1, k, h).start()
        mm((2, 3, 1))
        add_het(1, 0, 1)
        s2(2, 0, 1).start()
        mm((1, 3, 1))
        go_on(len(pending))

    variants = n_var * 128
    pl.run_scoped(features, pltpu.VMEM((SLOTS, 3, ROWS_IN, genes), jnp.int32))
    gene_margins()
    marg_pair(0).start()
    pl.run_scoped(
        products,
        pltpu.VMEM((2, samples, 128), BF16),
        pltpu.VMEM((4, 3, variants // 4, samples), BF16),
    )
    for h in range(2):
        add_total(1, h)
        s2(0, 1, h).start()
    add_het(3, 2, 0)
    s2(2, 1, 0).start()
    add_allelic(3, 1, 0)
    add_total(2, 0)
    add_total(2, 1)
    add_allelic(3, 1, 1)
    add_total(3, 0)
    add_het(3, 2, 1)
    s2(2, 1, 1).start()
    add_total(3, 1)
    for p in (2, 0, 1):
        pass_on(p, 0)
    for p in (2, 0, 1):
        pass_on(p, 1)

    gene_total = marg_total(0)
    variant_total = marg_total(1)
    gene_sum = gene_total[0:1]
    gene_sq = gene_total[1:2]
    lane = lax.broadcasted_iota(jnp.int32, (rows, marg.shape[3]), 1)
    row = lax.broadcasted_iota(jnp.int32, (rows, marg.shape[3]), 0)
    mine = lane == row + rows * s
    dos_sum = jnp.sum(jnp.where(mine, variant_total[0:1], 0.0), axis=1, keepdims=True)
    dos_sq = jnp.sum(jnp.where(mine, variant_total[1:2], 0.0), axis=1, keepdims=True)
    n = sample_count
    dosage_var = dos_sq - dos_sum * dos_sum / n
    gene_var = gene_sq - gene_sum * gene_sum / n
    with jax.named_scope("drain_first"):
        drain_first()
    mean = gene_sum / n
    scale = (n**0.5) / jnp.sqrt((dosage_var + 1.0) * (gene_var + 1.0))
    for h in range(2):
        cols = halves[h]
        allelic = last_add(1, h)
        het_weight = last_add(2, h)
        with jax.named_scope("fin_a"):
            za_ref[:, cols] = allelic / jnp.sqrt(het_weight + 1.0)
        if h == 1:
            all_sent(r2, s2s)
        total = last_add(0, h)
        at = slice(h * half, (h + 1) * half)
        with jax.named_scope("fin_t"):
            zt_ref[:, cols] = (total - dos_sum * mean[:, at]) * scale[:, at]

    with jax.named_scope("drain"):
        all_sent(r3, s3s)


def hand_over(zt_held, za_held, zt_ref, za_ref, sems):
    copies = (
        pltpu.make_async_copy(zt_held, zt_ref, sems.at[0]),
        pltpu.make_async_copy(za_held, za_ref, sems.at[1]),
    )
    for copy in copies:
        copy.start()
    for copy in copies:
        copy.wait()


def per_device(sample_count, hap_words, total_counts, allele_one, allele_two):
    n_var = lax.axis_size("var")
    words, block = hap_words.shape[1:]
    samples, genes = total_counts.shape
    variants = block * n_var
    rows = variants // 16
    dma = pltpu.SemaphoreType.DMA
    out = jax.ShapeDtypeStruct((rows, genes), F32)
    held = pl.pallas_call(
        functools.partial(kernel, n_var, float(sample_count)),
        out_shape=(out, out),
        in_specs=[pl.BlockSpec(memory_space=pltpu.HBM)] * 4,
        out_specs=(pl.BlockSpec(memory_space=pltpu.VMEM),) * 2,
        scratch_shapes=[
            pltpu.VMEM((n_var, 2, words, block), jnp.int32),
            pltpu.VMEM((3, samples, genes), BF16),
            pltpu.VMEM((2, 8, genes), F32),
            pltpu.VMEM((3, 4, 2, 2, rows, genes), F32),
            pltpu.VMEM((3, 4, 2, rows, genes), F32),
            pltpu.VMEM((3, 4, rows, genes), F32),
            pltpu.VMEM((3, 2, rows, genes), F32),
            pltpu.VMEM((3, rows, genes), F32),
            pltpu.VMEM((2, 2, 2, variants), F32),
            pltpu.VMEM((2, 8, 2, variants), F32),
            dma((SLOTS,)),
            dma,
            dma,
            dma((n_var,)),
            dma,
            dma((3, 8)),
            dma,
            dma((3, 8)),
            dma,
            dma((3, 2, 2)),
            dma,
            dma((3, 2)),
            dma,
            dma((2, 2)),
        ],
        compiler_params=pltpu.CompilerParams(
            collective_id=0,
            has_side_effects=True,
            vmem_limit_bytes=55_600_000,
        ),
    )(pltpu.with_memory_space_constraint(hap_words, pltpu.HBM), total_counts, allele_one, allele_two)
    return pl.pallas_call(
        hand_over,
        out_shape=(out, out),
        in_specs=[pl.BlockSpec(memory_space=pltpu.VMEM)] * 2,
        out_specs=(pl.BlockSpec(memory_space=pltpu.HBM),) * 2,
        scratch_shapes=[dma((2,))],
        compiler_params=pltpu.CompilerParams(vmem_limit_bytes=2_000_000),
    )(*held)


def solution(mesh):
    in_specs = (P(None, "samp", "var"), P("samp", "var"), P("samp", "var"), P("samp", "var"))
    out_specs = (P("samp", "var"), P("samp", "var"))

    def whole(hap_words, total_counts, allele_one, allele_two):
        body = functools.partial(per_device, total_counts.shape[0])
        return jax.shard_map(
            body, mesh=mesh, in_specs=in_specs, out_specs=out_specs, check_vma=False
        )(hap_words, total_counts, allele_one, allele_two)

    return whole
```

```python
import functools

import jax
import jax.numpy as jnp
from jax import lax
from jax.experimental import pallas as pl
from jax.experimental.pallas import tpu as pltpu
from jax.sharding import PartitionSpec as P

BITS = 30
ROWS_IN = 128
SLOTS = 6
TURN = 5
DEFER = 2
STEP = 16
SEND_AT = (0, 4, 8, 12)
FAR_FIRST = (5, 4, 7, 6, 1, 3, 2)
LANES = 256
MESH = pl.DeviceIdType.MESH
BF16 = jnp.bfloat16
F32 = jnp.float32


def kernel(
    n_var,
    sample_count,
    hap_ref,
    total_ref,
    one_ref,
    two_ref,
    zt_ref,
    za_ref,
    hall,
    feats,
    gacc,
    acc,
    r0,
    r1,
    r2,
    r3,
    marg,
    mrecv,
    in_sem,
    hap_own,
    hap_send,
    hap_recv,
    s0s,
    s0r,
    s1s,
    s1r,
    s2s,
    s2r,
    s3s,
    s3r,
    ms,
    mr,
):
    samples, genes = total_ref.shape
    words = hap_ref.shape[1]
    rows = acc.shape[4]
    s = lax.axis_index("samp")
    v = lax.axis_index("var")
    c = s % 2
    y = (s // 2) % 2
    z = s // 4
    x = v // 2
    za = z + 1 - 2 * (z % 2)
    zb = 3 - z
    zc = (z + 2) % 4
    core_dev = (s + 1 - 2 * c, v)
    y_dev = (s + 2 - 4 * y, v)
    a_dev = (za * 4 + y * 2 + c, v)
    b_dev = (zb * 4 + y * 2 + c, v)
    chips = [((s + 2 * j) % 16, v) for j in range(1, 8)]
    oc = 1 - c
    oy = 1 - y

    half = genes // 2
    halves = (pl.ds(0, half), pl.ds(half, half))

    n_chunks = samples // ROWS_IN

    def fetch(counts, k, slot, which, ref):
        at = pl.multiple_of(k * ROWS_IN, ROWS_IN)
        return pltpu.make_async_copy(
            ref.at[pl.ds(at, ROWS_IN), :],
            counts.at[slot, which],
            in_sem.at[slot],
        )

    sources = (total_ref, one_ref, two_ref)
    own = pltpu.make_async_copy(hap_ref, hall.at[v], hap_own)

    def peer(k, sign):
        return ((x + sign * (k // 2) + 4) % 4) * 2 + (v + k) % 2

    def hap_copy(k):
        return pltpu.make_async_remote_copy(
            src_ref=hap_ref,
            dst_ref=hall.at[v],
            send_sem=hap_send,
            recv_sem=hap_recv.at[k],
            device_id=(s, peer(k, 1)),
            device_id_type=MESH,
        )

    def hap_arrival(k):
        return pltpu.make_async_remote_copy(
            src_ref=hap_ref,
            dst_ref=hall.at[peer(k, -1)],
            send_sem=hap_send,
            recv_sem=hap_recv.at[k],
            device_id=(s, peer(k, 1)),
            device_id_type=MESH,
        )

    at_tile = [jnp.where(x == w, k, 0) for w, k in zip((zc, za, zb, z), SEND_AT)]
    send_at = sum(at_tile)

    gacc[...] = jnp.zeros_like(gacc)

    def chunk_step(counts, k, carry):
        slot = k % SLOTS

        @pl.when(k == send_at)
        def _():
            for m in FAR_FIRST:
                hap_copy(m).start()

        @pl.when(k + SLOTS - 1 < n_chunks)
        def _():
            for which, ref in enumerate(sources):
                fetch(counts, k + SLOTS - 1, (k + SLOTS - 1) % SLOTS, which, ref).start()

        pltpu.make_async_copy(counts.at[slot], counts.at[slot], in_sem.at[slot]).wait()
        def row_step(r, carry):
            at = pl.ds(pl.multiple_of(r * STEP, STEP), STEP)
            out = pl.ds(pl.multiple_of(k * ROWS_IN + r * STEP, STEP), STEP)
            for lane in range(0, genes, LANES):
                cols = pl.ds(lane, LANES)
                log_total = jnp.log((counts[slot, 0, at, cols] + 1).astype(F32))
                one = (counts[slot, 1, at, cols] + 1).astype(F32)
                two = (counts[slot, 2, at, cols] + 1).astype(F32)
                weight = (one * two) / (one + two)
                weighted = weight * (jnp.log(one) - jnp.log(two))
                feats[0, out, cols] = log_total.astype(BF16)
                feats[1, out, cols] = weighted.astype(BF16)
                feats[2, out, cols] = weight.astype(BF16)
                square = log_total * log_total
                gacc[0, :, cols] += log_total[:8] + log_total[8:]
                gacc[1, :, cols] += square[:8] + square[8:]
            return carry

        lax.fori_loop(0, ROWS_IN // STEP, row_step, 0, unroll=8)
        return carry

    def features(counts):
        barrier = pltpu.get_barrier_semaphore()
        for dev in (core_dev, *chips):
            pl.semaphore_signal(barrier, inc=1, device_id=dev, device_id_type=MESH)
        for k in range(1, n_var):
            pl.semaphore_signal(
                barrier, inc=1, device_id=(s, (v + k) % n_var), device_id_type=MESH
            )
        for k in range(SLOTS - 1):
            for which, ref in enumerate(sources):
                fetch(counts, k, k, which, ref).start()
        own.start()
        with jax.named_scope("barrier"):
            pl.semaphore_wait(barrier, 8 + n_var - 1)
        step = functools.partial(chunk_step, counts)
        with jax.named_scope("features"):
            lax.fori_loop(0, n_chunks, step, 0)

    def hap_wait(i):
        target = (zc, za, zb, z)[i]
        with jax.named_scope("hap_wait"):
            for b in range(2):
                k = ((x + 4 - target) % 4) * 2 + (v + b) % 2

                @pl.when(k == 0)
                def _():
                    own.wait()

                @pl.when(k != 0)
                def _():
                    hap_arrival(k).wait_recv()

    def gene_margins():
        marg[0, 0, 0:1, :] = jnp.sum(gacc[0], axis=0, keepdims=True)
        marg[0, 0, 1:2, :] = jnp.sum(gacc[1], axis=0, keepdims=True)

    def variant_margins():
        for b in range(n_var):
            w0, w1 = hall[b, 0], hall[b, 1]
            bits = lax.population_count(w0) + lax.population_count(w1)
            het = lax.population_count(jnp.bitwise_xor(w0, w1))
            cols = pl.ds(b * 128, 128)
            bit_sum = jnp.sum(bits.astype(F32), axis=0, keepdims=True)
            het_sum = jnp.sum(het.astype(F32), axis=0, keepdims=True)
            marg[1, 0, 0:1, cols] = bit_sum - float(samples)
            marg[1, 0, 1:2, cols] = float(samples) - het_sum

    def marg_pair(w):
        return pltpu.make_async_remote_copy(
            src_ref=marg.at[w, 0],
            dst_ref=mrecv.at[w, 0],
            send_sem=ms,
            recv_sem=mr.at[w, 0],
            device_id=core_dev,
            device_id_type=MESH,
        )

    def marg_chip(w, j):
        return pltpu.make_async_remote_copy(
            src_ref=marg.at[w, 1],
            dst_ref=mrecv.at[w, j],
            send_sem=ms,
            recv_sem=mr.at[w, 1],
            device_id=chips[j - 1],
            device_id_type=MESH,
        )

    def marg_share(w):
        with jax.named_scope("marg_wait"):
            marg_pair(w).wait_recv()
        marg[w, 1] = marg[w, 0] + mrecv[w, 0]
        for j in range(1, 8):
            marg_chip(w, j).start()

    def marg_total(w):
        others = mrecv.at[w, pl.ds(1, 7)]
        with jax.named_scope("marg_wait"):
            pltpu.make_async_copy(others, others, mr.at[w, 1]).wait()
        total = marg[w, 1]
        for j in range(1, 8):
            total = total + mrecv[w, j]
        return total

    def send(src, dst, ss, rs, dev):
        return pltpu.make_async_remote_copy(
            src_ref=src,
            dst_ref=dst,
            send_sem=ss,
            recv_sem=rs,
            device_id=dev,
            device_id_type=MESH,
        )

    def s0(p, i, g):
        cols = halves[g]
        return send(
            acc.at[p, i, :, oc, :, cols],
            r0.at[p, i, :, :, cols],
            s0s,
            s0r.at[p, 2 * i + g],
            core_dev,
        )

    def s1(p, i, g):
        cols = halves[g]
        if p == 0:
            src, dst, dev = acc.at[p, i, oy, c, :, cols], r1.at[p, i, :, cols], y_dev
        else:
            dev = a_dev if p == 1 else b_dev
            first = 2 * i if p == 1 else i
            src, dst = acc.at[p, i, :, c, :, cols], r1.at[p, pl.ds(first, 2), :, cols]
        return send(src, dst, s1s, s1r.at[p, 2 * i + g], dev)

    def goes_on(p, i):
        return p == 0 or (i < 2 if p == 1 else i % 2 == 0)

    def s0_finish(p, i, g):
        cols = halves[g]
        with jax.named_scope("s0_wait"):
            s0(p, i, g).wait_recv()
        for t in range(2):
            acc[p, i, t, c, :, cols] += r0[p, i, t, :, cols]
        if goes_on(p, i):
            s1(p, i, g).start()

    iota = lax.broadcasted_iota(jnp.int32, (8, 128), 0)

    def unpack_words(tbuf, i):
        zt = (zc, za, zb, z)[i]
        for b in range(2):
            block = 2 * zt + b

            def word_step(g, carry):
                at = pl.ds(pl.multiple_of(g * 8, 8), 8)
                w0 = hall[block, 0, at, :]
                w1 = hall[block, 1, at, :] << 1
                parts = []
                for t in range(BITS):
                    first = 8 * t // BITS
                    last = (8 * t + 7) // BITS
                    shift = iota + (8 * t - BITS * first)
                    u0 = jnp.broadcast_to(w0[first : first + 1], (8, 128))
                    u1 = jnp.broadcast_to(w1[first : first + 1], (8, 128))
                    if last != first:
                        early = iota < BITS * last - 8 * t
                        shift = jnp.where(early, shift, shift - BITS)
                        u0 = jnp.where(early, u0, jnp.broadcast_to(w0[last : last + 1], (8, 128)))
                        u1 = jnp.where(early, u1, jnp.broadcast_to(w1[last : last + 1], (8, 128)))
                    code = ((u0 >> shift) & 1) | ((u1 >> shift) & 2)
                    parts.append(code.astype(F32))
                out = pl.ds(pl.multiple_of(g * 8 * BITS, 16), 8 * BITS)
                tbuf[b, out, :] = jnp.concatenate(parts, axis=0).astype(BF16)
                return carry

            lax.fori_loop(0, words // 8, word_step, 0)

    def turn(tbuf, lhs, i):
        def turn_step(k, carry):
            for b in range(2):
                for j in range(TURN):
                    at = pl.ds(pl.multiple_of(k * (TURN * 128) + j * 128, 128), 128)
                    centred = tbuf[b, at, :].T - 1.5
                    het = jnp.abs(centred) < 1.0
                    zero = jnp.zeros_like(centred)
                    out = pl.ds(b * 128, 128)
                    lhs[i, 0, out, at] = jnp.clip(jnp.where(het, zero, centred), -1.0, 1.0)
                    lhs[i, 1, out, at] = jnp.where(het, centred * -2.0, zero)
                    lhs[i, 2, out, at] = jnp.where(het, jnp.ones_like(centred), zero)
            return carry

        lax.fori_loop(0, samples // (TURN * 128), turn_step, 0)

    def matmul(lhs, p, i, h):
        cols = halves[h]
        with jax.named_scope("matmul"):
            res = jnp.dot(lhs[i, p], feats[p, :, cols], preferred_element_type=F32)
            acc[p, i, :, :, :, cols] = res.reshape(2, 2, rows, res.shape[1])
        s0(p, i, h).start()

    def s2(p, k, h):
        if p == 0:
            src, dev = (k, y), a_dev
        elif p == 1:
            src, dev = (2, oy if k == 0 else y), b_dev
        else:
            src, dev = (1 + 2 * k, oy), y_dev
        return send(
            acc.at[p, src[0], src[1], c, :, halves[h]],
            r2.at[p, k, :, halves[h]],
            s2s,
            s2r.at[p, k, h],
            dev,
        )

    def s3(p, h):
        src, dev = (((2, y), b_dev), ((3, oy), y_dev), ((1, y), a_dev))[p]
        return send(
            acc.at[p, src[0], src[1], c, :, halves[h]],
            r3.at[p, :, halves[h]],
            s3s,
            s3r.at[p, h],
            dev,
        )

    def s1_arrival(p, i, h):
        with jax.named_scope(f"s1_{p}"):
            s1(p, i, h).wait_recv()

    def add_allelic(tile, k, h):
        s1_arrival(1, k, h)
        for t in range(2):
            acc[1, tile, t, c, :, halves[h]] += r1[1, 2 * k + t, :, halves[h]]

    def add_het(tile, k, h):
        s1_arrival(2, k, h)
        for t in range(2):
            acc[2, tile, t, c, :, halves[h]] += r1[2, k + t, :, halves[h]]

    def add_total(k, h):
        s1_arrival(0, k, h)
        acc[0, k, y, c, :, halves[h]] += r1[0, k, :, halves[h]]

    def pass_on(p, h):
        with jax.named_scope(f"s2_{p}_0"):
            s2(p, 0, h).wait_recv()
        tile, t = ((2, y), (3, oy), (1, y))[p]
        acc[p, tile, t, c, :, halves[h]] += r2[p, 0, :, halves[h]]
        s3(p, h).start()

    def last_add(p, h):
        with jax.named_scope(f"s2_{p}_1"):
            s2(p, 1, h).wait_recv()
        with jax.named_scope(f"s3_{p}"):
            s3(p, h).wait_recv()
        return acc[p, 3, y, c, :, halves[h]] + r2[p, 1, :, halves[h]] + r3[p, :, halves[h]]

    def all_sent(ref, sem):
        pltpu.make_async_copy(ref, ref, sem).wait()

    def drain_first():
        all_sent(hall.at[pl.ds(0, n_var - 1)], hap_send)
        all_sent(mrecv, ms)
        all_sent(r0, s0s)
        all_sent(r1, s1s)

    def products(tbuf, lhs):
        def words_of(i):
            hap_wait(i)
            with jax.named_scope("words"):
                unpack_words(tbuf, i)

        def turn_of(i):
            with jax.named_scope("turn"):
                turn(tbuf, lhs, i)

        pending = []

        def mm(*steps):
            for step in steps:
                matmul(lhs, *step)
                pending.append(step)
                if len(pending) > DEFER:
                    go_on(1)

        def go_on(count):
            for step in pending[:count]:
                s0_finish(*step)
            del pending[:count]

        words_of(0)
        marg_share(0)
        turn_of(0)
        for g in range(2):
            mm((0, 0, g), (1, 0, g), (2, 0, g))
        words_of(1)
        go_on(2)
        turn_of(1)
        mm((0, 1, 0), (0, 1, 1))
        words_of(2)
        go_on(2)
        turn_of(2)
        mm((0, 2, 0), (1, 1, 0), (2, 2, 0), (0, 2, 1))
        words_of(3)
        go_on(2)
        turn_of(3)
        variant_margins()
        marg_pair(1).start()
        mm((0, 3, 0), (1, 1, 1), (2, 2, 1), (0, 3, 1))
        marg_share(1)
        mm((1, 2, 0), (2, 1, 0), (1, 2, 1), (2, 1, 1))
        add_allelic(2, 0, 0)
        s2(1, 0, 0).start()
        add_total(0, 0)
        s2(0, 0, 0).start()
        mm((2, 3, 0),)
        add_het(1, 0, 0)
        s2(2, 0, 0).start()
        add_total(0, 1)
        s2(0, 0, 1).start()
        mm((1, 3, 0))
        add_allelic(2, 0, 1)
        for k, h in ((0, 1), (1, 0), (1, 1)):
            s2(1, k, h).start()
        mm((2, 3, 1))
        add_het(1, 0, 1)
        s2(2, 0, 1).start()
        mm((1, 3, 1))
        go_on(len(pending))

    variants = n_var * 128
    pl.run_scoped(features, pltpu.VMEM((SLOTS, 3, ROWS_IN, genes), jnp.int32))
    gene_margins()
    marg_pair(0).start()
    pl.run_scoped(
        products,
        pltpu.VMEM((2, samples, 128), BF16),
        pltpu.VMEM((4, 3, variants // 4, samples), BF16),
    )
    for h in range(2):
        add_total(1, h)
        s2(0, 1, h).start()
    add_het(3, 2, 0)
    s2(2, 1, 0).start()
    add_allelic(3, 1, 0)
    add_total(2, 0)
    add_total(2, 1)
    add_allelic(3, 1, 1)
    add_total(3, 0)
    add_het(3, 2, 1)
    s2(2, 1, 1).start()
    add_total(3, 1)
    for p in (2, 0, 1):
        pass_on(p, 0)
    for p in (2, 0, 1):
        pass_on(p, 1)

    gene_total = marg_total(0)
    variant_total = marg_total(1)
    gene_sum = gene_total[0:1]
    gene_sq = gene_total[1:2]
    lane = lax.broadcasted_iota(jnp.int32, (rows, marg.shape[3]), 1)
    row = lax.broadcasted_iota(jnp.int32, (rows, marg.shape[3]), 0)
    mine = lane == row + rows * s
    dos_sum = jnp.sum(jnp.where(mine, variant_total[0:1], 0.0), axis=1, keepdims=True)
    dos_sq = jnp.sum(jnp.where(mine, variant_total[1:2], 0.0), axis=1, keepdims=True)
    n = sample_count
    dosage_var = dos_sq - dos_sum * dos_sum / n
    gene_var = gene_sq - gene_sum * gene_sum / n
    with jax.named_scope("drain_first"):
        drain_first()
    mean = gene_sum / n
    scale = (n**0.5) / jnp.sqrt((dosage_var + 1.0) * (gene_var + 1.0))
    for h in range(2):
        cols = halves[h]
        allelic = last_add(1, h)
        het_weight = last_add(2, h)
        with jax.named_scope("fin_a"):
            za_ref[:, cols] = allelic / jnp.sqrt(het_weight + 1.0)
        if h == 1:
            all_sent(r2, s2s)
        total = last_add(0, h)
        at = slice(h * half, (h + 1) * half)
        with jax.named_scope("fin_t"):
            zt_ref[:, cols] = (total - dos_sum * mean[:, at]) * scale[:, at]

    with jax.named_scope("drain"):
        all_sent(r3, s3s)


def hand_over(zt_held, za_held, zt_ref, za_ref, sems):
    copies = (
        pltpu.make_async_copy(zt_held, zt_ref, sems.at[0]),
        pltpu.make_async_copy(za_held, za_ref, sems.at[1]),
    )
    for copy in copies:
        copy.start()
    for copy in copies:
        copy.wait()


def per_device(sample_count, hap_words, total_counts, allele_one, allele_two):
    n_var = lax.axis_size("var")
    words, block = hap_words.shape[1:]
    samples, genes = total_counts.shape
    variants = block * n_var
    rows = variants // 16
    dma = pltpu.SemaphoreType.DMA
    out = jax.ShapeDtypeStruct((rows, genes), F32)
    held = pl.pallas_call(
        functools.partial(kernel, n_var, float(sample_count)),
        out_shape=(out, out),
        in_specs=[pl.BlockSpec(memory_space=pltpu.HBM)] * 4,
        out_specs=(pl.BlockSpec(memory_space=pltpu.VMEM),) * 2,
        scratch_shapes=[
            pltpu.VMEM((n_var, 2, words, block), jnp.int32),
            pltpu.VMEM((3, samples, genes), BF16),
            pltpu.VMEM((2, 8, genes), F32),
            pltpu.VMEM((3, 4, 2, 2, rows, genes), F32),
            pltpu.VMEM((3, 4, 2, rows, genes), F32),
            pltpu.VMEM((3, 4, rows, genes), F32),
            pltpu.VMEM((3, 2, rows, genes), F32),
            pltpu.VMEM((3, rows, genes), F32),
            pltpu.VMEM((2, 2, 2, variants), F32),
            pltpu.VMEM((2, 8, 2, variants), F32),
            dma((SLOTS,)),
            dma,
            dma,
            dma((n_var,)),
            dma,
            dma((3, 8)),
            dma,
            dma((3, 8)),
            dma,
            dma((3, 2, 2)),
            dma,
            dma((3, 2)),
            dma,
            dma((2, 2)),
        ],
        compiler_params=pltpu.CompilerParams(
            collective_id=0,
            has_side_effects=True,
            vmem_limit_bytes=55_600_000,
        ),
    )(pltpu.with_memory_space_constraint(hap_words, pltpu.HBM), total_counts, allele_one, allele_two)
    return pl.pallas_call(
        hand_over,
        out_shape=(out, out),
        in_specs=[pl.BlockSpec(memory_space=pltpu.VMEM)] * 2,
        out_specs=(pl.BlockSpec(memory_space=pltpu.HBM),) * 2,
        scratch_shapes=[dma((2,))],
        compiler_params=pltpu.CompilerParams(vmem_limit_bytes=2_000_000),
    )(*held)


def solution(mesh):
    in_specs = (P(None, "samp", "var"), P("samp", "var"), P("samp", "var"), P("samp", "var"))
    out_specs = (P("samp", "var"), P("samp", "var"))

    def whole(hap_words, total_counts, allele_one, allele_two):
        body = functools.partial(per_device, total_counts.shape[0])
        return jax.shard_map(
            body, mesh=mesh, in_specs=in_specs, out_specs=out_specs, check_vma=False
        )(hap_words, total_counts, allele_one, allele_two)

    return whole
```
